32 devices in a mesh: gx: 8 (over z, y), gy: 4 (over x, core).
Axes of the slice: x: 2, y: 2, z: 4, core: 2. Of those that a mesh axis runs over, the one named last changes fastest.
Arguments:
- velocity: bfloat16 [3, 16, 16, 16, 512], P(None, 'gx', 'gy'), may hold values from -6 to 6
- part_pos: float32 [4096, 3, 128], P(('gx', 'gy')), may hold values from -1 to 1
- part_vel: float32 [4096, 3, 128], P(('gx', 'gy')), may hold values from -6 to 6
- part_coef: float32 [4096, 2, 128], P(('gx', 'gy')), may hold values from 0.3 to 3
- counts: int32 [4096], P(('gx', 'gy')), may hold values from 1 to 128
- dest: int32 [4096], P(('gx', 'gy')), may hold values from 0 to 3, as said below
- elem: int32 [4096], P(('gx', 'gy')), may hold values from 0 to 127, as said below
Outputs:
- drag: float32 [4096, 3, 128], P(('gx', 'gy'))
- source: float32 [3, 16, 16, 16, 512], P(None, 'gx', 'gy')
The draws below stay inside these ranges and needn't reach their ends.
Inputs may be any that keep to these rules, and one draw needn't show every extreme that they name: `dest`: every device sends exactly 32 blocks to each gy index. `elem`: on every owning device, each of its 128 elements receives exactly one block.
All inputs are finite; a program needn't handle non-finite values.
Results may differ from the reference program's by a relative error of at most 0.0003.
Values sent between devices are 32-bit elements; how exact they have to be, the bound alone decides.
A program may use at most 128 MiB of HBM per device.

```python
import math
import jax
import jax.numpy as jnp
from jax import lax

EXD = 2
EYD = 4
EZ = 16
NODES = 512
SLOTS = 128
E_DEV = 128
NEX = 16
NEY = 16
NB = 4096
N_GX = 8
N_GY = 4


def joint_routes(key):
    share_size = E_DEV // N_GY

    def one_row(row_key):
        elem_keys = jax.random.split(jax.random.fold_in(row_key, 1), N_GY)
        mix_keys = jax.random.split(jax.random.fold_in(row_key, 2), N_GY)
        ladder = jnp.arange(E_DEV, dtype=jnp.int32)
        incoming = jax.vmap(lambda k: jax.random.permutation(k, ladder))(elem_keys)
        elements = incoming.reshape(N_GY, N_GY, share_size).transpose(1, 0, 2).reshape(N_GY, E_DEV)
        targets = jnp.broadcast_to(jnp.arange(N_GY, dtype=jnp.int32)[None, :, None], (N_GY, N_GY, share_size)).reshape(N_GY, E_DEV)
        shuffle = jax.vmap(lambda k: jax.random.permutation(k, ladder))(mix_keys)
        return (jnp.take_along_axis(targets, shuffle, axis=1), jnp.take_along_axis(elements, shuffle, axis=1))
    targets, elements = jax.vmap(one_row)(jax.random.split(key, N_GX))
    return (targets.reshape(-1), elements.reshape(-1))


def draw_dest(key, part):
    return joint_routes(jax.random.fold_in(key, 7))[0]


def draw_elem(key, part):
    return joint_routes(jax.random.fold_in(key, 7))[1]


def set_ends(result, stream_key, low, high):
    extent = result.shape
    spot = [jax.random.randint(jax.random.fold_in(stream_key, axis), (), 0, extent[axis]) for axis in range(len(extent))]
    result = result.at[tuple(spot)].set(low)
    longest = extent.index(max(extent))
    spot[longest] = (spot[longest] + 1) % extent[longest]
    return result.at[tuple(spot)].set(high)


def block_scale(stream_key, extent, pieces, smallest, largest):
    def one(dim, parts):
        steps = jax.random.uniform(jax.random.fold_in(jax.random.fold_in(stream_key, 6), dim), (parts,), jnp.float32, smallest / len(pieces), largest / len(pieces))
        return jnp.repeat(jnp.exp(steps), extent[dim] // parts).reshape((-1,) + (1,) * (len(extent) - dim - 1))

    loudness = one(*pieces[0])
    for cut in pieces[1:]:
        loudness = loudness * one(*cut)
    return loudness


def scatter_about(key, shape, scale, most, cuts=(), kind=jnp.bfloat16):
    level = block_scale(key, shape, cuts, -0.22, 0.18) if cuts else 1.0
    drawn = jax.random.normal(key, shape, jnp.float32) * scale * level
    return jnp.minimum(jnp.maximum(drawn, -most), most).astype(kind)


def setup_inputs(seed: int = 0) -> dict:
    splits = jax.random.split(jax.random.key(seed), 8)
    return {
        "velocity": scatter_about(splits[0], (3, NEX, NEY, EZ, NODES), 1.0, 6.0, ((1, 8), (2, 4))),
        "part_pos": jnp.clip(jax.random.uniform(splits[1], (NB, 3, SLOTS), jnp.float32, -1.0, 1.0) * block_scale(splits[1], (NB, 3, SLOTS), ((0, 32),), -0.4, 0.0), -1.0, 1.0),
        "part_vel": scatter_about(splits[2], (NB, 3, SLOTS), 1.0, 6.0, ((0, 32),), jnp.float32),
        "part_coef": jnp.clip(jnp.exp(math.log(3.0) - 2.3025851 * jax.random.uniform(splits[3], (NB, 2, SLOTS), jnp.float32) ** block_scale(splits[3], (NB, 2, SLOTS), ((0, 32),), -0.2, 0.2)), 0.3, 3.0),
        "counts": set_ends(jax.random.randint(splits[4], (NB,), 1, 129), jax.random.fold_in(splits[4], 1), 1, 128).astype(jnp.int32),
        "dest": draw_dest(jax.random.fold_in(splits[7], 71), 0),
        "elem": draw_elem(jax.random.fold_in(splits[7], 71), 0),
    }


GLL = (-1.0, -0.8717401485096066, -0.5917001814331423, -0.2092992179024789, 0.2092992179024789, 0.5917001814331423, 0.8717401485096066, 1.0)
HIGH = lax.Precision.HIGHEST
SHARPNESS = 8.0

def lagrange_rows(coord):
    layers = []
    for i in range(8):
        product = jnp.ones_like(coord)
        for m in range(8):
            if m != i:
                product = product * ((coord - GLL[m]) / (GLL[i] - GLL[m]))
        layers.append(product)
    return jnp.stack(layers, axis=1)

def gauss_rows(coord, offset):
    points = jnp.array(GLL, dtype=jnp.float32)
    spacing = points[None, :, None] - (coord[:, None, :] + offset)
    return jnp.exp(-SHARPNESS * spacing * spacing)

def element_step(field, position, carried, coefs, filled):
    group = field.shape[0]
    width = position.shape[2]
    basis_r = lagrange_rows(position[:, 0])
    basis_s = lagrange_rows(position[:, 1])
    basis_t = lagrange_rows(position[:, 2])
    nodal = field.reshape(group, 3, 8, 64)
    partial_sum = jnp.einsum('gcia,gip->gcap', nodal, basis_r, precision=HIGH)
    planes = (basis_s[:, :, None, :] * basis_t[:, None, :, :]).reshape(group, 64, width)
    fluid = lax.optimization_barrier(jnp.sum(partial_sum * planes[:, None], axis=2))
    relative = fluid - carried
    speed = jnp.sqrt(lax.optimization_barrier(jnp.sum(relative * relative, axis=1)))
    factor = coefs[:, 0] * (1.0 + 0.15 * jnp.power(coefs[:, 1] * speed, 0.687))
    live = jnp.arange(width, dtype=jnp.int32)[None, :] < filled[:, None]
    drag = jnp.where(live[:, None, :], factor[:, None, :] * relative, jnp.zeros_like(relative))
    weights_s = gauss_rows(position[:, 1], 0.0)
    weights_t = gauss_rows(position[:, 2], 0.0)
    spread = (-drag)[:, :, None, None, :] * weights_s[:, None, :, None, :] * weights_t[:, None, None, :, :]
    spread = spread.reshape(group, 192, width)
    weights_r = jnp.stack([gauss_rows(position[:, 0], 0.0), gauss_rows(position[:, 0], 2.0), gauss_rows(position[:, 0], -2.0)], axis=1)
    deposit = jnp.einsum('gsip,gap->gsia', weights_r, spread, precision=HIGH)
    deposit = deposit.reshape(group, 3, 8, 3, 64).transpose(0, 1, 3, 2, 4).reshape(group, 3, 3, 512)
    return (drag, deposit)

def run_groups(field, position, carried, coefs, filled, group):
    total = field.shape[0]
    turns = total // group
    packed = tuple((a.reshape((turns, group) + a.shape[1:]) for a in (field, position, carried, coefs, filled)))
    drag, deposit = lax.map(lambda args: element_step(*args), packed)
    return (drag.reshape((total,) + drag.shape[2:]), deposit.reshape((total,) + deposit.shape[2:]))

def dss_axis(field, elem_axis, node_axis, far_lo, far_hi):
    count = field.shape[elem_axis]
    lower = lax.slice_in_dim(field, 0, 1, axis=node_axis)
    upper = lax.slice_in_dim(field, 7, 8, axis=node_axis)
    edge_shape = lax.slice_in_dim(lower, 0, 1, axis=elem_axis).shape
    lower_next = jnp.concatenate([lax.slice_in_dim(lower, 1, count, axis=elem_axis), far_lo.reshape(edge_shape)], axis=elem_axis)
    upper_prev = jnp.concatenate([far_hi.reshape(edge_shape), lax.slice_in_dim(upper, 0, count - 1, axis=elem_axis)], axis=elem_axis)
    middle = lax.slice_in_dim(field, 1, 7, axis=node_axis)
    return jnp.concatenate([lower + upper_prev, middle, upper + lower_next], axis=node_axis)

def edge_zeros(field, elem_axis, node_axis):
    edge = lax.slice_in_dim(lax.slice_in_dim(field, 0, 1, axis=elem_axis), 0, 1, axis=node_axis)
    return jnp.zeros_like(edge).reshape(-1)

def reference(velocity, part_pos, part_vel, part_coef, counts, dest, elem):
    blocks = part_pos.shape[0]
    source_row = jnp.arange(blocks, dtype=jnp.int32) // (E_DEV * N_GY)
    local_x = elem // (EYD * EZ)
    local_y = elem // EZ % EYD
    local_z = elem % EZ
    global_id = ((source_row * EXD + local_x) * NEY + dest * EYD + local_y) * EZ + local_z
    by_elem = jnp.argsort(global_id)
    field_e = velocity.reshape(3, blocks, NODES).transpose(1, 0, 2).astype(jnp.float32)
    drag_e, deposit = run_groups(field_e, part_pos[by_elem], part_vel[by_elem], part_coef[by_elem], counts[by_elem], math.gcd(blocks, 256))
    drag = drag_e[global_id]
    deposit = deposit.transpose(1, 2, 0, 3).reshape(3, 3, NEX, NEY, EZ, 8, 8, 8)
    own_part, minus_part, plus_part = (deposit[0], deposit[1], deposit[2])
    empty_layer = jnp.zeros_like(own_part[:, 0:1])
    total = own_part + jnp.concatenate([minus_part[:, 1:], empty_layer], axis=1) + jnp.concatenate([empty_layer, plus_part[:, :-1]], axis=1)
    field = total
    for elem_axis, node_axis in ((1, 4), (2, 5), (3, 6)):
        zeros_edge = edge_zeros(field, elem_axis, node_axis)
        field = dss_axis(field, elem_axis, node_axis, zeros_edge, zeros_edge)
    return (drag, field.reshape(3, NEX, NEY, EZ, NODES))
```

```python
import functools

import jax
import jax.numpy as jnp
from jax import lax
from jax.experimental import pallas as pl
from jax.experimental.pallas import tpu as pltpu
from jax.sharding import PartitionSpec as P

GLL = (
    -1.0,
    -0.8717401485096066,
    -0.5917001814331423,
    -0.2092992179024789,
    0.2092992179024789,
    0.5917001814331423,
    0.8717401485096066,
    1.0,
)
SHARPNESS = 8.0
VMEM = pltpu.VMEM
SMEM = pltpu.SMEM
ROWS = 24


def lane_iota(shape):
    return lax.broadcasted_iota(jnp.int32, shape, len(shape) - 1)


def node_consts():
    row = lax.broadcasted_iota(jnp.int32, (8, 128), 0)

    def pick(values):
        out = jnp.full((8, 128), values[7], jnp.float32)
        for i in range(7):
            out = jnp.where(row == i, jnp.float32(values[i]), out)
        return out

    others = [pick([[GLL[m] for m in range(8) if m != i][n] for i in range(8)]) for n in range(7)]
    scales = []
    for i in range(8):
        product = 1.0
        for m in range(8):
            if m != i:
                product *= GLL[i] - GLL[m]
        scales.append(1.0 / product)
    return pick(GLL), others, pick(scales)


def lagrange(x, others, scale):
    diffs = [x - o for o in others]
    left = (diffs[0] * diffs[1]) * (diffs[2] * diffs[3])
    right = (diffs[4] * diffs[5]) * (diffs[6] * scale)
    return left * right


def gauss(x, nodes):
    gap = nodes - x
    return jnp.exp(-SHARPNESS * gap * gap)


def split(x):
    high = x.astype(jnp.bfloat16)
    low = (x - high.astype(jnp.float32)).astype(jnp.bfloat16)
    return high, low


def planes(a, b):
    return jnp.concatenate([a[j : j + 1] * b for j in range(8)], axis=0)


def spread_nodes(vel_ref, vs_ref, elems):
    low = lane_iota((elems, 128)) < 64
    for c in range(3):
        for q in range(4):
            x = vel_ref[c, :, q * 128 : (q + 1) * 128].astype(jnp.float32)
            turned = pltpu.roll(x, 64, 1)
            vs_ref[pl.ds(c * 8 + 2 * q, elems, stride=ROWS), :] = jnp.where(low, x, turned)
            vs_ref[pl.ds(c * 8 + 2 * q + 1, elems, stride=ROWS), :] = jnp.where(low, turned, x)


def element(block, count, field, consts):
    nodes, others, scale = consts
    r, s, t = (jnp.broadcast_to(block[d : d + 1], (8, 128)) for d in range(3))
    basis_r = lagrange(r, others, scale)
    basis_st = planes(lagrange(s, others, scale), lagrange(t, others, scale))
    high, low = split(basis_st)
    partial = jnp.dot(
        field.astype(jnp.bfloat16),
        jnp.concatenate([high, low], axis=0),
        preferred_element_type=jnp.float32,
    )
    rel = []
    for c in range(3):
        fluid = jnp.sum(partial[c * 8 : c * 8 + 8] * basis_r, axis=0, keepdims=True)
        rel.append(fluid - block[3 + c : 4 + c])
    speed = jnp.sqrt(rel[0] * rel[0] + rel[1] * rel[1] + rel[2] * rel[2])
    power = jnp.exp(0.687 * jnp.log(block[7:8] * speed))
    factor = block[6:7] * (1.0 + 0.15 * power)
    factor = jnp.where(lane_iota((1, 128)) < count, factor, 0.0)
    drag = [factor * w for w in rel]
    g_high, g_low = split(planes(gauss(s, nodes), gauss(t, nodes)))
    gathered = jnp.concatenate([g_high, g_low], axis=0)
    weights = [gauss(r, nodes), gauss(r + 2.0, nodes), gauss(r - 2.0, nodes)]
    left = jnp.concatenate([(-d) * w for w in weights for d in drag], axis=0)
    l_high, l_low = split(left)
    deposit = lax.dot_general(
        jnp.concatenate([l_high, l_low], axis=1),
        jnp.concatenate([gathered, gathered], axis=1),
        (((1,), (1,)), ((), ())),
        preferred_element_type=jnp.float32,
    )
    return jnp.concatenate(drag, axis=0), deposit


def compute_kernel(
    exd, slot_ref, count_ref, got_ref, vel_ref,
    drag_ref, total_ref, prev_ref, next_ref,
    vs_ref, ts_ref, gm_ref, gp_ref,
):
    elems = vel_ref.shape[1]
    columns = elems // exd
    group = 4 if columns % 4 == 0 else 1
    spread_nodes(vel_ref, vs_ref, elems)
    consts = node_consts()

    def turn(index, carry):
        for g in range(group):
            col = index * group + g
            deposits = []
            for x in range(exd):
                e = x * columns + col
                slot = slot_ref[e]
                drag, deposit = element(
                    got_ref[slot],
                    count_ref[slot],
                    vs_ref[pl.ds(pl.multiple_of(e * ROWS, 8), ROWS), :],
                    consts,
                )
                drag_ref[slot] = drag
                deposits.append(deposit)
            for x in range(exd):
                e = x * columns + col
                own = deposits[x][0:ROWS]
                if x + 1 < exd:
                    own = own + deposits[x + 1][ROWS : 2 * ROWS]
                if x > 0:
                    own = own + deposits[x - 1][2 * ROWS :]
                ts_ref[pl.ds(pl.multiple_of(e * ROWS, 8), ROWS), :] = own
            start = pl.multiple_of(col * ROWS, 8)
            gm_ref[pl.ds(start, ROWS), :] = deposits[0][ROWS : 2 * ROWS]
            gp_ref[pl.ds(start, ROWS), :] = deposits[exd - 1][2 * ROWS :]
        return carry

    lax.fori_loop(0, columns // group, turn, 0)

    def lanes(src, count, c, q):
        low = lane_iota((count, 128)) < 64
        even = src[pl.ds(c * 8 + 2 * q, count, stride=ROWS), :]
        odd = src[pl.ds(c * 8 + 2 * q + 1, count, stride=ROWS), :]
        mine = jnp.where(low, even, odd)
        other = jnp.where(low, odd, even)
        return mine + pltpu.roll(other, 64, 1)

    for c in range(3):
        for q in range(4):
            spot = slice(q * 128, (q + 1) * 128)
            total = lanes(ts_ref, elems, c, q)
            total_ref[c, :, spot] = total
            prev_ref[c, :, spot] = lanes(gm_ref, columns, c, q)
            next_ref[c, :, spot] = lanes(gp_ref, columns, c, q)
            if q == 0:
                prev_ref[c, :, 512:640] = total[0:columns]
            if q == 3:
                next_ref[c, :, 512:640] = total[elems - columns :]


def run_compute(slot, count, got, velocity, exd):
    elems = velocity.shape[1]
    columns = elems // exd
    f32 = jnp.float32
    return pl.pallas_call(
        functools.partial(compute_kernel, exd),
        out_shape=(
            jax.ShapeDtypeStruct((elems, 3, 128), f32),
            jax.ShapeDtypeStruct((3, elems, 512), f32),
            jax.ShapeDtypeStruct((3, columns, 640), f32),
            jax.ShapeDtypeStruct((3, columns, 640), f32),
        ),
        in_specs=[
            pl.BlockSpec(memory_space=SMEM),
            pl.BlockSpec(memory_space=SMEM),
            pl.BlockSpec(memory_space=VMEM),
            pl.BlockSpec(memory_space=VMEM),
        ],
        out_specs=[pl.BlockSpec(memory_space=VMEM)] * 4,
        scratch_shapes=[
            pltpu.VMEM((elems * ROWS, 128), f32),
            pltpu.VMEM((elems * ROWS, 128), f32),
            pltpu.VMEM((columns * ROWS, 128), f32),
            pltpu.VMEM((columns * ROWS, 128), f32),
        ],
        compiler_params=pltpu.CompilerParams(vmem_limit_bytes=48 * 1024 * 1024),
        cost_estimate=pl.CostEstimate(flops=200_000_000, bytes_accessed=4_000_000, transcendentals=700_000),
        name="elements",
    )(slot, count, got, velocity)


def x_pass(total_ref, prev_ref, next_ref, from_prev, from_next, field_ref, lo_ref, hi_ref):
    _, exd, eyd, ez, _ = total_ref.shape
    at = lax.axis_index("gx")
    first = jnp.where(at > 0, 1.0, 0.0)
    last = jnp.where(at < lax.axis_size("gx") - 1, 1.0, 0.0)
    low = lane_iota((ez, 128)) < 64
    place = lane_iota((ez, 128)) % 64

    def column(c, y):
        rows = slice(y * ez, (y + 1) * ez)
        grid = []
        for x in range(exd):
            quads = []
            for q in range(4):
                spot = slice(q * 128, (q + 1) * 128)
                v = total_ref[c, x, y, :, spot]
                if x == 0:
                    v = v + from_prev[c, rows, spot] * first
                if x == exd - 1:
                    v = v + from_next[c, rows, spot] * last
                quads.append(v)
            grid.append(quads)
        far_lo = (from_next[c, rows, 512:640] + next_ref[c, rows, 0:128]) * last
        far_hi = (from_prev[c, rows, 512:640] + prev_ref[c, rows, 384:512]) * first
        for x in range(exd):
            above = grid[x + 1][0] if x + 1 < exd else far_lo
            below = grid[x - 1][3] if x > 0 else far_hi
            done = list(grid[x])
            done[3] = done[3] + jnp.where(low, 0.0, pltpu.roll(above, 64, 1))
            done[0] = done[0] + jnp.where(low, pltpu.roll(below, 64, 1), 0.0)
            for q in range(4):
                field_ref[c, x, y, :, q * 128 : (q + 1) * 128] = done[q]
            if y == 0:
                face = jnp.where(place < 8, done[0], 0.0)
                for q in range(1, 4):
                    face = face + pltpu.roll(jnp.where(place < 8, done[q], 0.0), 8 * q, 1)
                lo_ref[c, x] = face
            if y == eyd - 1:
                face = jnp.where(place >= 56, done[0], 0.0)
                for q in range(1, 4):
                    face = face + pltpu.roll(jnp.where(place >= 56, done[q], 0.0), 128 - 8 * q, 1)
                hi_ref[c, x] = face

    for c in range(3):
        for y in range(eyd):
            column(c, y)


def yz_pass(field_ref, far_lo_ref, far_hi_ref, out_ref):
    _, exd, eyd, ez, _ = field_ref.shape
    at = lax.axis_index("gy")
    first = jnp.where(at > 0, 1.0, 0.0)
    last = jnp.where(at < lax.axis_size("gy") - 1, 1.0, 0.0)
    place = lane_iota((ez, 128)) % 64
    k = lane_iota((ez, 128)) % 8
    row = lax.broadcasted_iota(jnp.int32, (ez, 128), 0)
    up = (k == 7) & (row < ez - 1)
    down = (k == 0) & (row > 0)
    for c in range(3):
        for x in range(exd):
            far_lo = far_lo_ref[c, x] * last
            far_hi = far_hi_ref[c, x] * first
            for q in range(4):
                spot = slice(q * 128, (q + 1) * 128)
                cells = [field_ref[c, x, y, :, spot] for y in range(eyd)]
                for y in range(eyd):
                    if y + 1 < eyd:
                        above = pltpu.roll(cells[y + 1], 56, 1)
                    else:
                        above = pltpu.roll(far_lo, (56 - 8 * q) % 128, 1)
                    if y > 0:
                        below = pltpu.roll(cells[y - 1], 72, 1)
                    else:
                        below = pltpu.roll(far_hi, (72 + 8 * q) % 128, 1)
                    v = cells[y] + jnp.where(place >= 56, above, 0.0) + jnp.where(place < 8, below, 0.0)
                    nxt = pltpu.roll(pltpu.roll(v, ez - 1, 0), 7, 1)
                    prv = pltpu.roll(pltpu.roll(v, 1, 0), 121, 1)
                    out_ref[c, x, y, :, spot] = v + jnp.where(up, nxt, 0.0) + jnp.where(down, prv, 0.0)


def run_local(body, outs, *args, name):
    return pl.pallas_call(
        body,
        out_shape=outs,
        in_specs=[pl.BlockSpec(memory_space=VMEM)] * len(args),
        out_specs=jax.tree.map(lambda _: pl.BlockSpec(memory_space=VMEM), outs),
        compiler_params=pltpu.CompilerParams(vmem_limit_bytes=48 * 1024 * 1024),
        name=name,
    )(*args)


def shifted(shard, axis, by):
    count = lax.axis_size(axis)
    pairs = [(i, i + by) for i in range(count) if 0 <= i + by < count]
    return lax.ppermute(shard, axis, pairs)


def inverse_of(position):
    n = position.shape[0]
    ladder = jnp.arange(n, dtype=jnp.int32)
    return jnp.sum(jnp.where(position[None, :] == ladder[:, None], ladder[None, :], 0), axis=1)


def body(velocity, part_pos, part_vel, part_coef, counts, dest, elem):
    _, exd, eyd, ez, nodes = velocity.shape
    elems = exd * eyd * ez
    devices = lax.axis_size("gy")
    share = elems // devices
    f32 = jnp.float32
    ladder = jnp.arange(elems, dtype=jnp.int32)
    earlier = (dest[None, :] == dest[:, None]) & (ladder[None, :] < ladder[:, None])
    position = dest * share + jnp.sum(earlier.astype(jnp.int32), axis=1)
    sorting = inverse_of(position)
    packed = jnp.concatenate([part_pos, part_vel, part_coef], axis=1)[sorting]
    labels = (elem * 256 + counts)[sorting].astype(f32)
    got = lax.all_to_all(packed, "gy", split_axis=0, concat_axis=0, tiled=True)
    got_labels = lax.all_to_all(labels.reshape(devices, share), "gy", split_axis=0, concat_axis=0, tiled=True)
    got_labels = got_labels.reshape(elems).astype(jnp.int32)
    slot = inverse_of(got_labels // 256)
    drag_slots, total, to_prev, to_next = run_compute(
        slot, got_labels % 256, got, velocity.reshape(3, elems, nodes), exd
    )
    returned = lax.all_to_all(drag_slots, "gy", split_axis=0, concat_axis=0, tiled=True)
    drag_out = returned[position]
    from_next = shifted(to_prev, "gx", -1)
    from_prev = shifted(to_next, "gx", 1)
    cube = jax.ShapeDtypeStruct((3, exd, eyd, ez, nodes), f32)
    face = jax.ShapeDtypeStruct((3, exd, ez, 128), f32)
    field, lo, hi = run_local(
        x_pass, (cube, face, face),
        total.reshape(cube.shape), to_prev, to_next, from_prev, from_next, name="xpass",
    )
    far_lo = shifted(lo, "gy", -1)
    far_hi = shifted(hi, "gy", 1)
    source = run_local(yz_pass, cube, field, far_lo, far_hi, name="yzpass")
    return (drag_out, source)


def solution(mesh):
    in_specs = (
        P(None, "gx", "gy", None, None),
        P(("gx", "gy"), None, None),
        P(("gx", "gy"), None, None),
        P(("gx", "gy"), None, None),
        P(("gx", "gy")),
        P(("gx", "gy")),
        P(("gx", "gy")),
    )
    out_specs = (P(("gx", "gy"), None, None), P(None, "gx", "gy", None, None))
    return jax.shard_map(body, mesh=mesh, in_specs=in_specs, out_specs=out_specs, check_vma=False)
```

```python
import functools

import jax
import jax.numpy as jnp
from jax import lax
from jax.experimental import pallas as pl
from jax.experimental.pallas import tpu as pltpu
from jax.sharding import PartitionSpec as P

GLL = (
    -1.0,
    -0.8717401485096066,
    -0.5917001814331423,
    -0.2092992179024789,
    0.2092992179024789,
    0.5917001814331423,
    0.8717401485096066,
    1.0,
)
SHARPNESS = 8.0
VMEM = pltpu.VMEM
SMEM = pltpu.SMEM
ROWS = 24


def lane_iota(shape):
    return lax.broadcasted_iota(jnp.int32, shape, len(shape) - 1)


def node_consts():
    row = lax.broadcasted_iota(jnp.int32, (8, 128), 0)

    def pick(values):
        out = jnp.full((8, 128), values[7], jnp.float32)
        for i in range(7):
            out = jnp.where(row == i, jnp.float32(values[i]), out)
        return out

    others = [pick([[GLL[m] for m in range(8) if m != i][n] for i in range(8)]) for n in range(7)]
    scales = []
    for i in range(8):
        product = 1.0
        for m in range(8):
            if m != i:
                product *= GLL[i] - GLL[m]
        scales.append(1.0 / product)
    return pick(GLL), others, pick(scales)


def lagrange(x, others, scale):
    diffs = [x - o for o in others]
    left = (diffs[0] * diffs[1]) * (diffs[2] * diffs[3])
    right = (diffs[4] * diffs[5]) * (diffs[6] * scale)
    return left * right


def gauss(x, nodes):
    gap = nodes - x
    return jnp.exp(-SHARPNESS * gap * gap)


def split(x):
    high = x.astype(jnp.bfloat16)
    low = (x - high.astype(jnp.float32)).astype(jnp.bfloat16)
    return high, low


def planes(a, b):
    return jnp.concatenate([a[j : j + 1] * b for j in range(8)], axis=0)


def spread_nodes(vel_ref, vs_ref, elems):
    low = lane_iota((elems, 128)) < 64
    for c in range(3):
        for q in range(4):
            x = vel_ref[c, :, q * 128 : (q + 1) * 128].astype(jnp.float32)
            turned = pltpu.roll(x, 64, 1)
            vs_ref[pl.ds(c * 8 + 2 * q, elems, stride=ROWS), :] = jnp.where(low, x, turned)
            vs_ref[pl.ds(c * 8 + 2 * q + 1, elems, stride=ROWS), :] = jnp.where(low, turned, x)


def st_planes(s, t, nodes):
    high, low = split(planes(gauss(s, nodes), gauss(t, nodes)))
    gathered = jnp.concatenate([high, low], axis=0)
    return jnp.concatenate([gathered, gathered], axis=1)


def project(left, gathered):
    high, low = split(left)
    return lax.dot_general(
        jnp.concatenate([high, low], axis=1),
        gathered,
        (((1,), (1,)), ((), ())),
        preferred_element_type=jnp.float32,
    )


def element(block, count, field, consts, inner_minus, inner_plus):
    nodes, others, scale = consts
    r, s, t = (jnp.broadcast_to(block[d : d + 1], (8, 128)) for d in range(3))
    basis_r = lagrange(r, others, scale)
    basis_st = planes(lagrange(s, others, scale), lagrange(t, others, scale))
    high, low = split(basis_st)
    partial = jnp.dot(
        field.astype(jnp.bfloat16),
        jnp.concatenate([high, low], axis=0),
        preferred_element_type=jnp.float32,
    )
    rel = []
    for c in range(3):
        fluid = jnp.sum(partial[c * 8 : c * 8 + 8] * basis_r, axis=0, keepdims=True)
        rel.append(fluid - block[3 + c : 4 + c])
    speed = jnp.sqrt(rel[0] * rel[0] + rel[1] * rel[1] + rel[2] * rel[2])
    power = jnp.exp(0.687 * jnp.log(block[7:8] * speed))
    factor = block[6:7] * (1.0 + 0.15 * power)
    factor = jnp.where(lane_iota((1, 128)) < count, factor, 0.0)
    drag = [factor * w for w in rel]
    whole = jnp.concatenate(drag, axis=0)
    minus = gauss(r + 2.0, nodes)
    plus = gauss(r - 2.0, nodes)
    weights = [gauss(r, nodes)]
    if inner_minus:
        weights.append(minus)
    if inner_plus:
        weights.append(plus)
    rows = [(-d) * w for w in weights for d in drag]
    blank = jnp.zeros((5, 128), jnp.float32)
    if not inner_minus:
        rows.append(jnp.concatenate([-whole * minus[7:8], blank], axis=0))
    if not inner_plus:
        rows.append(jnp.concatenate([-whole * plus[0:1], blank], axis=0))
    out = project(jnp.concatenate(rows, axis=0), st_planes(s, t, nodes))
    parts, at = {}, ROWS
    parts["own"] = out[0:ROWS]
    for name, inner in (("minus", inner_minus), ("plus", inner_plus)):
        if inner:
            parts[name] = out[at : at + ROWS]
            at += ROWS
    for name, inner in (("minus", inner_minus), ("plus", inner_plus)):
        if not inner:
            parts[name] = out[at : at + 8]
            at += 8
    return whole, parts


def main_kernel(
    shape, chunks, n_gx, n_gy,
    slot_ref, count_ref, elem_ref, got_ref, vel_ref,
    field_ref, far_lo_ref, far_hi_ref, ret_ref,
    vs_ref, ts_ref, fs_ref, drag_ref, pos_ref, gpos_ref, gdrag_ref,
    face_ref, gface_ref, lo_ref, hi_ref, back_ref,
    pos_sem, drag_sem, face_sem, y_sem, back_sem,
):
    exd, eyd, ez = shape
    elems = exd * eyd * ez
    columns = eyd * ez
    share = elems // n_gy
    group = 4
    turns = columns // group
    per = turns // chunks
    wide = columns // chunks
    half = columns // 2
    gx = lax.axis_index("gx")
    gy = lax.axis_index("gy")
    has = (gx > 0, gx < n_gx - 1)
    mesh_id = pl.DeviceIdType.MESH

    def to_side(side, src, dst, sems, *at):
        return pltpu.make_async_remote_copy(
            src_ref=src, dst_ref=dst,
            send_sem=sems.at[(0, side) + at], recv_sem=sems.at[(1, 1 - side) + at],
            device_id={"gx": gx - 1 if side == 0 else gx + 1}, device_id_type=mesh_id,
        )

    def from_side(side, src, dst, sems, *at):
        return pltpu.make_async_remote_copy(
            src_ref=src, dst_ref=dst,
            send_sem=sems.at[(0, side) + at], recv_sem=sems.at[(1, side) + at],
            device_id={"gx": gx - 1 if side == 0 else gx + 1}, device_id_type=mesh_id,
        )

    barrier = pltpu.get_barrier_semaphore()
    for side in range(2):
        @pl.when(has[side])
        def _():
            pl.semaphore_signal(
                barrier, inc=1, device_id={"gx": gx - 1 if side == 0 else gx + 1}, device_id_type=mesh_id
            )
    for off in range(1, n_gy):
        pl.semaphore_signal(
            barrier, inc=1, device_id={"gy": lax.rem(gy + off, n_gy)}, device_id_type=mesh_id
        )

    base = (0, elems - columns)

    def stage(col, carry):
        for side in range(2):
            pos_ref[side, col] = got_ref[slot_ref[base[side] + col], 0:3]
        return carry

    lax.fori_loop(0, columns, stage, 0, unroll=4)
    pl.semaphore_wait(
        barrier, n_gy - 1 + (gx > 0).astype(jnp.int32) + (gx < n_gx - 1).astype(jnp.int32)
    )
    for side in range(2):
        @pl.when(has[side])
        def _():
            to_side(side, pos_ref.at[side], gpos_ref.at[1 - side], pos_sem).start()

    spread_nodes(vel_ref, vs_ref, elems)
    consts = node_consts()
    nodes = consts[0]

    def drag_copy(make, side, chunk):
        start = base[side] + chunk * wide
        return make(
            side, drag_ref.at[pl.ds(start, wide)], gdrag_ref.at[1 - side, pl.ds(chunk * wide, wide)], drag_sem, chunk
        )

    def turn(index, carry):
        for g in range(group):
            col = index * group + g
            parts = []
            for x in range(exd):
                e = x * columns + col
                slot = slot_ref[e]
                drag, part = element(
                    got_ref[slot],
                    count_ref[slot],
                    vs_ref[pl.ds(pl.multiple_of(e * ROWS, 8), ROWS), :],
                    consts,
                    x > 0,
                    x + 1 < exd,
                )
                drag_ref[e] = drag
                parts.append(part)
            for x in range(exd):
                e = x * columns + col
                own = parts[x]["own"]
                if x + 1 < exd:
                    own = own + parts[x + 1]["minus"]
                if x > 0:
                    own = own + parts[x - 1]["plus"]
                ts_ref[pl.ds(pl.multiple_of(e * ROWS, 8), ROWS), :] = own
            start = pl.multiple_of(col * 8, 8)
            fs_ref[0, pl.ds(start, 8), :] = parts[0]["minus"]
            fs_ref[1, pl.ds(start, 8), :] = parts[exd - 1]["plus"]
        for side in range(2):
            @pl.when((lax.rem(index, per) == per - 1) & has[side])
            def _():
                drag_copy(to_side, side, lax.div(index, per)).start()
        return carry

    lax.fori_loop(0, turns, turn, 0)

    def doubled(x):
        return x + pltpu.roll(x, 64, 1)

    low_h = lane_iota((half, 128)) < 64
    for side in range(2):
        node = 0 if side == 0 else 7
        for c in range(3):
            one = doubled(ts_ref[pl.ds(base[side] * ROWS + c * 8 + node, half, stride=ROWS), :])
            two = doubled(ts_ref[pl.ds((base[side] + half) * ROWS + c * 8 + node, half, stride=ROWS), :])
            face_ref[side, c] = jnp.where(low_h, one, two)
        @pl.when(has[side])
        def _():
            to_side(side, face_ref.at[side], gface_ref.at[1 - side], face_sem).start()

    def fill(k, carry):
        back_ref[k] = drag_ref[elem_ref[k]]
        return carry

    lax.fori_loop(0, elems, fill, 0, unroll=4)

    def back_copy(off):
        peer = lax.rem(gy + off, n_gy)
        return pltpu.make_async_remote_copy(
            src_ref=back_ref.at[pl.ds(peer * share, share)], dst_ref=ret_ref.at[pl.ds(gy * share, share)],
            send_sem=back_sem.at[0, off - 1], recv_sem=back_sem.at[1, off - 1],
            device_id={"gy": peer}, device_id_type=mesh_id,
        )

    for off in range(1, n_gy):
        back_copy(off).start()

    def keep(k, carry):
        ret_ref[gy * share + k] = back_ref[gy * share + k]
        return carry

    lax.fori_loop(0, share, keep, 0, unroll=4)

    for side in range(2):
        @pl.when(has[side])
        def _():
            from_side(side, pos_ref.at[side], gpos_ref.at[side], pos_sem).wait()

        def ghost(index, carry):
            @pl.when(lax.rem(index, per) == 0)
            def _():
                chunk = lax.div(index, per)
                from_side(
                    side, drag_ref.at[pl.ds(base[side] + chunk * wide, wide)],
                    gdrag_ref.at[side, pl.ds(chunk * wide, wide)], drag_sem, chunk,
                ).wait()

            for g in range(group):
                col = index * group + g
                place = gpos_ref[side, col]
                force = gdrag_ref[side, col]
                r, s, t = (jnp.broadcast_to(place[d : d + 1], (8, 128)) for d in range(3))
                weight = gauss(r + (-2.0 if side == 0 else 2.0), nodes)
                rows = [(-force[c : c + 1]) * weight for c in range(3)]
                add = project(jnp.concatenate(rows, axis=0), st_planes(s, t, nodes))
                spot = pl.ds(pl.multiple_of((base[side] + col) * ROWS, 8), ROWS)
                ts_ref[spot, :] = ts_ref[spot, :] + add
            return carry

        @pl.when(has[side])
        def _():
            lax.fori_loop(0, turns, ghost, 0)

    for side in range(2):
        @pl.when(has[side])
        def _():
            from_side(side, face_ref.at[side], gface_ref.at[side], face_sem).wait()

    low = lane_iota((ez, 128)) < 64
    spot64 = lane_iota((ez, 128)) % 64

    def lanes(c, x, y, q):
        start = ((x * eyd + y) * ez) * ROWS + c * 8 + 2 * q
        even = ts_ref[pl.ds(start, ez, stride=ROWS), :]
        odd = ts_ref[pl.ds(start + 1, ez, stride=ROWS), :]
        return jnp.where(low, even, odd) + pltpu.roll(jnp.where(low, odd, even), 64, 1)

    def far(side, c, y):
        col = y * ez
        upper = col >= half
        row = col - half if upper else col
        came = gface_ref[side, c, row : row + ez, :]
        turned = pltpu.roll(came, 64, 1)
        came = jnp.where(low, turned, came) if upper else jnp.where(low, came, turned)
        mine = doubled(fs_ref[side, pl.ds(col * 8 + c, ez, stride=8), :])
        return jnp.where(has[side], came + mine, 0.0)

    for y in (0, eyd - 1) + tuple(range(1, eyd - 1)):
        for c in range(3):
            grid = [[lanes(c, x, y, q) for q in range(4)] for x in range(exd)]
            for x in range(exd):
                above = pltpu.roll(grid[x + 1][0], 64, 1) if x + 1 < exd else far(1, c, y)
                below = pltpu.roll(grid[x - 1][3], 64, 1) if x > 0 else far(0, c, y)
                done = list(grid[x])
                done[3] = done[3] + jnp.where(low, 0.0, above)
                done[0] = done[0] + jnp.where(low, below, 0.0)
                for q in range(4):
                    field_ref[c, x, y, :, q * 128 : (q + 1) * 128] = done[q]
                if y == 0:
                    face = jnp.where(spot64 < 8, done[0], 0.0)
                    for q in range(1, 4):
                        face = face + pltpu.roll(jnp.where(spot64 < 8, done[q], 0.0), 8 * q, 1)
                    lo_ref[c, x] = face
                if y == eyd - 1:
                    face = jnp.where(spot64 >= 56, done[0], 0.0)
                    for q in range(1, 4):
                        face = face + pltpu.roll(jnp.where(spot64 >= 56, done[q], 0.0), 128 - 8 * q, 1)
                    hi_ref[c, x] = face
        if y == eyd - 1:
            lo_copy = pltpu.make_async_remote_copy(
                src_ref=lo_ref, dst_ref=far_lo_ref, send_sem=y_sem.at[0, 0], recv_sem=y_sem.at[1, 0],
                device_id={"gy": gy - 1}, device_id_type=mesh_id,
            )
            hi_copy = pltpu.make_async_remote_copy(
                src_ref=hi_ref, dst_ref=far_hi_ref, send_sem=y_sem.at[0, 1], recv_sem=y_sem.at[1, 1],
                device_id={"gy": gy + 1}, device_id_type=mesh_id,
            )
            @pl.when(gy > 0)
            def _():
                lo_copy.start()
            @pl.when(gy < n_gy - 1)
            def _():
                hi_copy.start()

    @pl.when(gy > 0)
    def _():
        lo_copy.wait_send()
        hi_copy.wait_recv()
    @pl.when(gy < n_gy - 1)
    def _():
        hi_copy.wait_send()
        lo_copy.wait_recv()
    for off in range(1, n_gy):
        back_copy(off).wait()


def run_main(slot, count, elem_of, got, velocity, shape):
    exd, eyd, ez = shape
    elems = exd * eyd * ez
    columns = eyd * ez
    n_gx, n_gy = lax.axis_size("gx"), lax.axis_size("gy")
    chunks = 4
    f32 = jnp.float32
    dma = pltpu.SemaphoreType.DMA
    face = (3, exd, ez, 128)
    return pl.pallas_call(
        functools.partial(main_kernel, shape, chunks, n_gx, n_gy),
        out_shape=(
            jax.ShapeDtypeStruct((3, exd, eyd, ez, 512), f32),
            jax.ShapeDtypeStruct(face, f32),
            jax.ShapeDtypeStruct(face, f32),
            jax.ShapeDtypeStruct((elems, 3, 128), f32),
        ),
        in_specs=[pl.BlockSpec(memory_space=SMEM)] * 3 + [pl.BlockSpec(memory_space=VMEM)] * 2,
        out_specs=[pl.BlockSpec(memory_space=VMEM)] * 4,
        scratch_shapes=[
            pltpu.VMEM((elems * ROWS, 128), f32),
            pltpu.VMEM((elems * ROWS, 128), f32),
            pltpu.VMEM((2, columns * 8, 128), f32),
            pltpu.VMEM((elems, 3, 128), f32),
            pltpu.VMEM((2, columns, 3, 128), f32),
            pltpu.VMEM((2, columns, 3, 128), f32),
            pltpu.VMEM((2, columns, 3, 128), f32),
            pltpu.VMEM((2, 3, columns // 2, 128), f32),
            pltpu.VMEM((2, 3, columns // 2, 128), f32),
            pltpu.VMEM(face, f32),
            pltpu.VMEM(face, f32),
            pltpu.VMEM((elems, 3, 128), f32),
            dma((2, 2)),
            dma((2, 2, chunks)),
            dma((2, 2)),
            dma((2, 2)),
            dma((2, n_gy - 1)),
        ],
        compiler_params=pltpu.CompilerParams(
            vmem_limit_bytes=48 * 1024 * 1024, collective_id=0, has_side_effects=True
        ),
        cost_estimate=pl.CostEstimate(flops=200_000_000, bytes_accessed=4_000_000, transcendentals=700_000),
        name="elements",
    )(slot, count, elem_of, got, velocity)


def yz_pass(position_ref, field_ref, far_lo_ref, far_hi_ref, ret_ref, out_ref, drag_ref, buf_ref, sem):
    _, exd, eyd, ez, _ = field_ref.shape
    at = lax.axis_index("gy")
    first = at > 0
    last = at < lax.axis_size("gy") - 1
    place = lane_iota((ez, 128)) % 64
    k = lane_iota((ez, 128)) % 8
    row = lax.broadcasted_iota(jnp.int32, (ez, 128), 0)
    up = (k == 7) & (row < ez - 1)
    down = (k == 0) & (row > 0)
    copies = []
    for c in range(3):
        for x in range(exd):
            far_lo = jnp.where(last, far_lo_ref[c, x], 0.0)
            far_hi = jnp.where(first, far_hi_ref[c, x], 0.0)
            for q in range(4):
                spot = slice(q * 128, (q + 1) * 128)
                cells = [field_ref[c, x, y, :, spot] for y in range(eyd)]
                for y in range(eyd):
                    if y + 1 < eyd:
                        above = pltpu.roll(cells[y + 1], 56, 1)
                    else:
                        above = pltpu.roll(far_lo, (56 - 8 * q) % 128, 1)
                    if y > 0:
                        below = pltpu.roll(cells[y - 1], 72, 1)
                    else:
                        below = pltpu.roll(far_hi, (72 + 8 * q) % 128, 1)
                    v = cells[y] + jnp.where(place >= 56, above, 0.0) + jnp.where(place < 8, below, 0.0)
                    nxt = pltpu.roll(pltpu.roll(v, ez - 1, 0), 7, 1)
                    prv = pltpu.roll(pltpu.roll(v, 1, 0), 121, 1)
                    buf_ref[c, x, y, :, spot] = v + jnp.where(up, nxt, 0.0) + jnp.where(down, prv, 0.0)


            copies.append(pltpu.make_async_copy(buf_ref.at[c, x], out_ref.at[c, x], sem.at[c, x]))
            copies[-1].start()

    def pick(b, carry):
        drag_ref[b] = ret_ref[position_ref[b]]
        return carry

    lax.fori_loop(0, ret_ref.shape[0], pick, 0, unroll=4)
    for copy in copies:
        copy.wait()


def run_yz(position, field, far_lo, far_hi, ret):
    f32 = jnp.float32
    return pl.pallas_call(
        yz_pass,
        out_shape=(jax.ShapeDtypeStruct(field.shape, f32), jax.ShapeDtypeStruct(ret.shape, f32)),
        in_specs=[pl.BlockSpec(memory_space=SMEM)] + [pl.BlockSpec(memory_space=VMEM)] * 4,
        out_specs=[pl.BlockSpec(memory_space=pl.ANY), pl.BlockSpec(memory_space=VMEM)],
        scratch_shapes=[pltpu.VMEM(field.shape, f32), pltpu.SemaphoreType.DMA(field.shape[:2])],
        compiler_params=pltpu.CompilerParams(vmem_limit_bytes=32 * 1024 * 1024),
        name="yzpass",
    )(position, field, far_lo, far_hi, ret)


def inverse_of(position):
    n = position.shape[0]
    ladder = jnp.arange(n, dtype=jnp.int32)
    return jnp.sum(jnp.where(position[None, :] == ladder[:, None], ladder[None, :], 0), axis=1)


def body(velocity, part_pos, part_vel, part_coef, counts, dest, elem):
    _, exd, eyd, ez, nodes = velocity.shape
    elems = exd * eyd * ez
    devices = lax.axis_size("gy")
    share = elems // devices
    f32 = jnp.float32
    ladder = jnp.arange(elems, dtype=jnp.int32)
    earlier = (dest[None, :] == dest[:, None]) & (ladder[None, :] < ladder[:, None])
    position = dest * share + jnp.sum(earlier.astype(jnp.int32), axis=1)
    sorting = inverse_of(position)
    packed = jnp.concatenate([part_pos, part_vel, part_coef], axis=1)[sorting]
    labels = (elem * 256 + counts)[sorting].astype(f32)
    got = lax.all_to_all(packed, "gy", split_axis=0, concat_axis=0, tiled=True)
    got_labels = lax.all_to_all(labels.reshape(devices, share), "gy", split_axis=0, concat_axis=0, tiled=True)
    got_labels = got_labels.reshape(elems).astype(jnp.int32)
    slot = inverse_of(got_labels // 256)
    field, far_lo, far_hi, ret = run_main(
        slot, got_labels % 256, got_labels // 256, got,
        velocity.reshape(3, elems, nodes), (exd, eyd, ez),
    )
    source, drag_out = run_yz(position, field, far_lo, far_hi, ret)
    return (drag_out, source)


def solution(mesh):
    in_specs = (
        P(None, "gx", "gy", None, None),
        P(("gx", "gy"), None, None),
        P(("gx", "gy"), None, None),
        P(("gx", "gy"), None, None),
        P(("gx", "gy")),
        P(("gx", "gy")),
        P(("gx", "gy")),
    )
    out_specs = (P(("gx", "gy"), None, None), P(None, "gx", "gy", None, None))
    return jax.shard_map(body, mesh=mesh, in_specs=in_specs, out_specs=out_specs, check_vma=False)
```

```python
import functools

import jax
import jax.numpy as jnp
from jax import lax
from jax.experimental import pallas as pl
from jax.experimental.pallas import tpu as pltpu
from jax.sharding import PartitionSpec as P

GLL = (
    -1.0,
    -0.8717401485096066,
    -0.5917001814331423,
    -0.2092992179024789,
    0.2092992179024789,
    0.5917001814331423,
    0.8717401485096066,
    1.0,
)
SHARPNESS = 8.0
VMEM = pltpu.VMEM
SMEM = pltpu.SMEM
ROWS = 24


def lane_iota(shape):
    return lax.broadcasted_iota(jnp.int32, shape, len(shape) - 1)


def node_consts():
    row = lax.broadcasted_iota(jnp.int32, (8, 128), 0)

    def pick(values):
        out = jnp.full((8, 128), values[7], jnp.float32)
        for i in range(7):
            out = jnp.where(row == i, jnp.float32(values[i]), out)
        return out

    others = [pick([[GLL[m] for m in range(8) if m != i][n] for i in range(8)]) for n in range(7)]
    scales = []
    for i in range(8):
        product = 1.0
        for m in range(8):
            if m != i:
                product *= GLL[i] - GLL[m]
        scales.append(1.0 / product)
    return pick(GLL), others, pick(scales)


def lagrange(x, others, scale):
    diffs = [x - o for o in others]
    left = (diffs[0] * diffs[1]) * (diffs[2] * diffs[3])
    right = (diffs[4] * diffs[5]) * (diffs[6] * scale)
    return left * right


def gauss(x, nodes):
    gap = nodes - x
    return jnp.exp(-SHARPNESS * gap * gap)


def split(x):
    high = x.astype(jnp.bfloat16)
    low = (x - high.astype(jnp.float32)).astype(jnp.bfloat16)
    return high, low


def planes(a, b):
    return jnp.concatenate([a[j : j + 1] * b for j in range(8)], axis=0)


def spread_nodes(vel_ref, vs_ref, elems):
    low = lane_iota((elems, 128)) < 64
    for c in range(3):
        for q in range(4):
            x = vel_ref[c, :, q * 128 : (q + 1) * 128].astype(jnp.float32)
            turned = pltpu.roll(x, 64, 1)
            vs_ref[pl.ds(c * 8 + 2 * q, elems, stride=ROWS), :] = jnp.where(low, x, turned)
            vs_ref[pl.ds(c * 8 + 2 * q + 1, elems, stride=ROWS), :] = jnp.where(low, turned, x)


def st_planes(s, t, nodes):
    high, low = split(planes(gauss(s, nodes), gauss(t, nodes)))
    gathered = jnp.concatenate([high, low], axis=0)
    return jnp.concatenate([gathered, gathered], axis=1)


def project(left, gathered):
    high, low = split(left)
    return lax.dot_general(
        jnp.concatenate([high, low], axis=1),
        gathered,
        (((1,), (1,)), ((), ())),
        preferred_element_type=jnp.float32,
    )


def element(block, count, field, consts, inner_minus, inner_plus):
    nodes, others, scale = consts
    r, s, t = (jnp.broadcast_to(block[d : d + 1], (8, 128)) for d in range(3))
    basis_r = lagrange(r, others, scale)
    basis_st = planes(lagrange(s, others, scale), lagrange(t, others, scale))
    high, low = split(basis_st)
    partial = jnp.dot(
        field.astype(jnp.bfloat16),
        jnp.concatenate([high, low], axis=0),
        preferred_element_type=jnp.float32,
    )
    rel = []
    for c in range(3):
        fluid = jnp.sum(partial[c * 8 : c * 8 + 8] * basis_r, axis=0, keepdims=True)
        rel.append(fluid - block[3 + c : 4 + c])
    speed = jnp.sqrt(rel[0] * rel[0] + rel[1] * rel[1] + rel[2] * rel[2])
    power = jnp.exp(0.687 * jnp.log(block[7:8] * speed))
    factor = block[6:7] * (1.0 + 0.15 * power)
    factor = jnp.where(lane_iota((1, 128)) < count, factor, 0.0)
    drag = [factor * w for w in rel]
    whole = jnp.concatenate(drag, axis=0)
    minus = gauss(r + 2.0, nodes)
    plus = gauss(r - 2.0, nodes)
    weights = [gauss(r, nodes)]
    if inner_minus:
        weights.append(minus)
    if inner_plus:
        weights.append(plus)
    rows = [(-d) * w for w in weights for d in drag]
    blank = jnp.zeros((5, 128), jnp.float32)
    if not inner_minus:
        rows.append(jnp.concatenate([-whole * minus[7:8], blank], axis=0))
    if not inner_plus:
        rows.append(jnp.concatenate([-whole * plus[0:1], blank], axis=0))
    out = project(jnp.concatenate(rows, axis=0), st_planes(s, t, nodes))
    parts, at = {}, ROWS
    parts["own"] = out[0:ROWS]
    for name, inner in (("minus", inner_minus), ("plus", inner_plus)):
        if inner:
            parts[name] = out[at : at + ROWS]
            at += ROWS
    for name, inner in (("minus", inner_minus), ("plus", inner_plus)):
        if not inner:
            parts[name] = out[at : at + 8]
            at += 8
    return whole, parts


def main_kernel(
    shape, chunks, n_gx, n_gy,
    slot_ref, count_ref, elem_ref, got_ref, vel_ref,
    field_ref, far_lo_ref, far_hi_ref, ret_ref,
    vs_ref, ts_ref, fs_ref, drag_ref, pos_ref, gpos_ref, gdrag_ref,
    face_ref, gface_ref, lo_ref, hi_ref, back_ref,
    pos_sem, drag_sem, face_sem, y_sem, back_sem,
):
    exd, eyd, ez = shape
    elems = exd * eyd * ez
    columns = eyd * ez
    share = elems // n_gy
    group = 4
    turns = columns // group
    per = turns // chunks
    wide = columns // chunks
    half = columns // 2
    gx = lax.axis_index("gx")
    gy = lax.axis_index("gy")
    has = (gx > 0, gx < n_gx - 1)
    mesh_id = pl.DeviceIdType.MESH

    def to_side(side, src, dst, sems, *at):
        return pltpu.make_async_remote_copy(
            src_ref=src, dst_ref=dst,
            send_sem=sems.at[(0, side) + at], recv_sem=sems.at[(1, 1 - side) + at],
            device_id={"gx": gx - 1 if side == 0 else gx + 1}, device_id_type=mesh_id,
        )

    def from_side(side, src, dst, sems, *at):
        return pltpu.make_async_remote_copy(
            src_ref=src, dst_ref=dst,
            send_sem=sems.at[(0, side) + at], recv_sem=sems.at[(1, side) + at],
            device_id={"gx": gx - 1 if side == 0 else gx + 1}, device_id_type=mesh_id,
        )

    barrier = pltpu.get_barrier_semaphore()
    for side in range(2):
        @pl.when(has[side])
        def _():
            pl.semaphore_signal(
                barrier, inc=1, device_id={"gx": gx - 1 if side == 0 else gx + 1}, device_id_type=mesh_id
            )
    for off in range(1, n_gy):
        pl.semaphore_signal(
            barrier, inc=1, device_id={"gy": lax.rem(gy + off, n_gy)}, device_id_type=mesh_id
        )

    base = (0, elems - columns)

    def stage(index, carry):
        spots = [(side, index * 4 + u) for side in range(2) for u in range(4)]
        held = [got_ref[slot_ref[base[side] + col], 0:3] for side, col in spots]
        for (side, col), value in zip(spots, held):
            pos_ref[side, col] = value
        return carry

    lax.fori_loop(0, columns // 4, stage, 0)
    pl.semaphore_wait(
        barrier, n_gy - 1 + (gx > 0).astype(jnp.int32) + (gx < n_gx - 1).astype(jnp.int32)
    )
    for side in range(2):
        @pl.when(has[side])
        def _():
            to_side(side, pos_ref.at[side], gpos_ref.at[1 - side], pos_sem).start()

    spread_nodes(vel_ref, vs_ref, elems)
    consts = node_consts()
    nodes = consts[0]

    def drag_copy(make, side, chunk):
        start = base[side] + chunk * wide
        return make(
            side, drag_ref.at[pl.ds(start, wide)], gdrag_ref.at[1 - side, pl.ds(chunk * wide, wide)], drag_sem, chunk
        )

    def turn(index, carry):
        for g in range(group):
            col = index * group + g
            parts = []
            for x in range(exd):
                e = x * columns + col
                slot = slot_ref[e]
                drag, part = element(
                    got_ref[slot],
                    count_ref[slot],
                    vs_ref[pl.ds(pl.multiple_of(e * ROWS, 8), ROWS), :],
                    consts,
                    x > 0,
                    x + 1 < exd,
                )
                drag_ref[e] = drag
                parts.append(part)
            for x in range(exd):
                e = x * columns + col
                own = parts[x]["own"]
                if x + 1 < exd:
                    own = own + parts[x + 1]["minus"]
                if x > 0:
                    own = own + parts[x - 1]["plus"]
                ts_ref[pl.ds(pl.multiple_of(e * ROWS, 8), ROWS), :] = own
            start = pl.multiple_of(col * 8, 8)
            fs_ref[0, pl.ds(start, 8), :] = parts[0]["minus"]
            fs_ref[1, pl.ds(start, 8), :] = parts[exd - 1]["plus"]
        for side in range(2):
            @pl.when((lax.rem(index, per) == per - 1) & has[side])
            def _():
                drag_copy(to_side, side, lax.div(index, per)).start()
        return carry

    lax.fori_loop(0, turns, turn, 0)

    def doubled(x):
        return x + pltpu.roll(x, 64, 1)

    low_h = lane_iota((half, 128)) < 64
    for side in range(2):
        node = 0 if side == 0 else 7
        for c in range(3):
            one = doubled(ts_ref[pl.ds(base[side] * ROWS + c * 8 + node, half, stride=ROWS), :])
            two = doubled(ts_ref[pl.ds((base[side] + half) * ROWS + c * 8 + node, half, stride=ROWS), :])
            face_ref[side, c] = jnp.where(low_h, one, two)
        @pl.when(has[side])
        def _():
            to_side(side, face_ref.at[side], gface_ref.at[1 - side], face_sem).start()

    def fill(index, carry):
        held = [drag_ref[elem_ref[index * 8 + u]] for u in range(8)]
        for u in range(8):
            back_ref[index * 8 + u] = held[u]
        return carry

    lax.fori_loop(0, elems // 8, fill, 0)

    def back_copy(off):
        peer = lax.rem(gy + off, n_gy)
        return pltpu.make_async_remote_copy(
            src_ref=back_ref.at[pl.ds(peer * share, share)], dst_ref=ret_ref.at[pl.ds(gy * share, share)],
            send_sem=back_sem.at[0, off - 1], recv_sem=back_sem.at[1, off - 1],
            device_id={"gy": peer}, device_id_type=mesh_id,
        )

    for off in range(1, n_gy):
        back_copy(off).start()

    mine = pl.ds(gy * share, share)
    ret_ref[mine] = back_ref[mine]

    for side in range(2):
        @pl.when(has[side])
        def _():
            from_side(side, pos_ref.at[side], gpos_ref.at[side], pos_sem).wait()

        def ghost(index, carry):
            @pl.when(lax.rem(index, per) == 0)
            def _():
                chunk = lax.div(index, per)
                from_side(
                    side, drag_ref.at[pl.ds(base[side] + chunk * wide, wide)],
                    gdrag_ref.at[side, pl.ds(chunk * wide, wide)], drag_sem, chunk,
                ).wait()

            for g in range(group):
                col = index * group + g
                place = gpos_ref[side, col]
                force = gdrag_ref[side, col]
                r, s, t = (jnp.broadcast_to(place[d : d + 1], (8, 128)) for d in range(3))
                weight = gauss(r + (-2.0 if side == 0 else 2.0), nodes)
                rows = [(-force[c : c + 1]) * weight for c in range(3)]
                add = project(jnp.concatenate(rows, axis=0), st_planes(s, t, nodes))
                spot = pl.ds(pl.multiple_of((base[side] + col) * ROWS, 8), ROWS)
                ts_ref[spot, :] = ts_ref[spot, :] + add
            return carry

        @pl.when(has[side])
        def _():
            lax.fori_loop(0, turns, ghost, 0)

    for side in range(2):
        @pl.when(has[side])
        def _():
            from_side(side, face_ref.at[side], gface_ref.at[side], face_sem).wait()

    low = lane_iota((ez, 128)) < 64
    spot64 = lane_iota((ez, 128)) % 64

    def lanes(c, x, y, q):
        start = ((x * eyd + y) * ez) * ROWS + c * 8 + 2 * q
        even = ts_ref[pl.ds(start, ez, stride=ROWS), :]
        odd = ts_ref[pl.ds(start + 1, ez, stride=ROWS), :]
        return jnp.where(low, even, odd) + pltpu.roll(jnp.where(low, odd, even), 64, 1)

    def far(side, c, y):
        col = y * ez
        upper = col >= half
        row = col - half if upper else col
        came = gface_ref[side, c, row : row + ez, :]
        turned = pltpu.roll(came, 64, 1)
        came = jnp.where(low, turned, came) if upper else jnp.where(low, came, turned)
        mine = doubled(fs_ref[side, pl.ds(col * 8 + c, ez, stride=8), :])
        return jnp.where(has[side], came + mine, 0.0)

    for y in (0, eyd - 1) + tuple(range(1, eyd - 1)):
        for c in range(3):
            grid = [[lanes(c, x, y, q) for q in range(4)] for x in range(exd)]
            for x in range(exd):
                above = pltpu.roll(grid[x + 1][0], 64, 1) if x + 1 < exd else far(1, c, y)
                below = pltpu.roll(grid[x - 1][3], 64, 1) if x > 0 else far(0, c, y)
                done = list(grid[x])
                done[3] = done[3] + jnp.where(low, 0.0, above)
                done[0] = done[0] + jnp.where(low, below, 0.0)
                for q in range(4):
                    field_ref[c, x, y, :, q * 128 : (q + 1) * 128] = done[q]
                if y == 0:
                    face = jnp.where(spot64 < 8, done[0], 0.0)
                    for q in range(1, 4):
                        face = face + pltpu.roll(jnp.where(spot64 < 8, done[q], 0.0), 8 * q, 1)
                    lo_ref[c, x] = face
                if y == eyd - 1:
                    face = jnp.where(spot64 >= 56, done[0], 0.0)
                    for q in range(1, 4):
                        face = face + pltpu.roll(jnp.where(spot64 >= 56, done[q], 0.0), 128 - 8 * q, 1)
                    hi_ref[c, x] = face
        if y == eyd - 1:
            lo_copy = pltpu.make_async_remote_copy(
                src_ref=lo_ref, dst_ref=far_lo_ref, send_sem=y_sem.at[0, 0], recv_sem=y_sem.at[1, 0],
                device_id={"gy": gy - 1}, device_id_type=mesh_id,
            )
            hi_copy = pltpu.make_async_remote_copy(
                src_ref=hi_ref, dst_ref=far_hi_ref, send_sem=y_sem.at[0, 1], recv_sem=y_sem.at[1, 1],
                device_id={"gy": gy + 1}, device_id_type=mesh_id,
            )
            @pl.when(gy > 0)
            def _():
                lo_copy.start()
            @pl.when(gy < n_gy - 1)
            def _():
                hi_copy.start()

    @pl.when(gy > 0)
    def _():
        lo_copy.wait_send()
        hi_copy.wait_recv()
    @pl.when(gy < n_gy - 1)
    def _():
        hi_copy.wait_send()
        lo_copy.wait_recv()
    for off in range(1, n_gy):
        back_copy(off).wait()


def run_main(slot, count, elem_of, got, velocity, shape):
    exd, eyd, ez = shape
    elems = exd * eyd * ez
    columns = eyd * ez
    n_gx, n_gy = lax.axis_size("gx"), lax.axis_size("gy")
    chunks = 4
    f32 = jnp.float32
    dma = pltpu.SemaphoreType.DMA
    face = (3, exd, ez, 128)
    return pl.pallas_call(
        functools.partial(main_kernel, shape, chunks, n_gx, n_gy),
        out_shape=(
            jax.ShapeDtypeStruct((3, exd, eyd, ez, 512), f32),
            jax.ShapeDtypeStruct(face, f32),
            jax.ShapeDtypeStruct(face, f32),
            jax.ShapeDtypeStruct((elems, 3, 128), f32),
        ),
        in_specs=[pl.BlockSpec(memory_space=SMEM)] * 3 + [pl.BlockSpec(memory_space=VMEM)] * 2,
        out_specs=[pl.BlockSpec(memory_space=VMEM)] * 4,
        scratch_shapes=[
            pltpu.VMEM((elems * ROWS, 128), f32),
            pltpu.VMEM((elems * ROWS, 128), f32),
            pltpu.VMEM((2, columns * 8, 128), f32),
            pltpu.VMEM((elems, 3, 128), f32),
            pltpu.VMEM((2, columns, 3, 128), f32),
            pltpu.VMEM((2, columns, 3, 128), f32),
            pltpu.VMEM((2, columns, 3, 128), f32),
            pltpu.VMEM((2, 3, columns // 2, 128), f32),
            pltpu.VMEM((2, 3, columns // 2, 128), f32),
            pltpu.VMEM(face, f32),
            pltpu.VMEM(face, f32),
            pltpu.VMEM((elems, 3, 128), f32),
            dma((2, 2)),
            dma((2, 2, chunks)),
            dma((2, 2)),
            dma((2, 2)),
            dma((2, n_gy - 1)),
        ],
        compiler_params=pltpu.CompilerParams(
            vmem_limit_bytes=48 * 1024 * 1024, collective_id=0, has_side_effects=True
        ),
        cost_estimate=pl.CostEstimate(flops=200_000_000, bytes_accessed=4_000_000, transcendentals=700_000),
        name="elements",
    )(slot, count, elem_of, got, velocity)


def yz_pass(position_ref, field_ref, far_lo_ref, far_hi_ref, ret_ref, out_ref, drag_ref, buf_ref, sem):
    _, exd, eyd, ez, _ = field_ref.shape
    at = lax.axis_index("gy")
    first = at > 0
    last = at < lax.axis_size("gy") - 1
    place = lane_iota((ez, 128)) % 64
    k = lane_iota((ez, 128)) % 8
    row = lax.broadcasted_iota(jnp.int32, (ez, 128), 0)
    up = (k == 7) & (row < ez - 1)
    down = (k == 0) & (row > 0)
    copies = []
    for c in range(3):
        for x in range(exd):
            far_lo = jnp.where(last, far_lo_ref[c, x], 0.0)
            far_hi = jnp.where(first, far_hi_ref[c, x], 0.0)
            for q in range(4):
                spot = slice(q * 128, (q + 1) * 128)
                cells = [field_ref[c, x, y, :, spot] for y in range(eyd)]
                for y in range(eyd):
                    if y + 1 < eyd:
                        above = pltpu.roll(cells[y + 1], 56, 1)
                    else:
                        above = pltpu.roll(far_lo, (56 - 8 * q) % 128, 1)
                    if y > 0:
                        below = pltpu.roll(cells[y - 1], 72, 1)
                    else:
                        below = pltpu.roll(far_hi, (72 + 8 * q) % 128, 1)
                    v = cells[y] + jnp.where(place >= 56, above, 0.0) + jnp.where(place < 8, below, 0.0)
                    nxt = pltpu.roll(pltpu.roll(v, ez - 1, 0), 7, 1)
                    prv = pltpu.roll(pltpu.roll(v, 1, 0), 121, 1)
                    buf_ref[c, x, y, :, spot] = v + jnp.where(up, nxt, 0.0) + jnp.where(down, prv, 0.0)


            copies.append(pltpu.make_async_copy(buf_ref.at[c, x], out_ref.at[c, x], sem.at[c, x]))
            copies[-1].start()

    def pick(index, carry):
        held = [ret_ref[position_ref[index * 8 + u]] for u in range(8)]
        for c in range(3):
            rows = jnp.concatenate([h[c : c + 1] for h in held], axis=0)
            drag_ref[c, pl.ds(pl.multiple_of(index * 8, 8), 8), :] = rows
        return carry

    lax.fori_loop(0, ret_ref.shape[0] // 8, pick, 0)
    for copy in copies:
        copy.wait()


def run_yz(position, field, far_lo, far_hi, ret):
    f32 = jnp.float32
    return pl.pallas_call(
        yz_pass,
        out_shape=(jax.ShapeDtypeStruct(field.shape, f32), jax.ShapeDtypeStruct((3, ret.shape[0], 128), f32)),
        in_specs=[pl.BlockSpec(memory_space=SMEM)] + [pl.BlockSpec(memory_space=VMEM)] * 4,
        out_specs=[pl.BlockSpec(memory_space=pl.ANY), pl.BlockSpec(memory_space=VMEM)],
        scratch_shapes=[pltpu.VMEM(field.shape, f32), pltpu.SemaphoreType.DMA(field.shape[:2])],
        compiler_params=pltpu.CompilerParams(vmem_limit_bytes=32 * 1024 * 1024),
        name="yzpass",
    )(position, field, far_lo, far_hi, ret)


def send_kernel(
    n_gy, sorting_ref, pos_ref, vel_ref, coef_ref, label_ref,
    got_ref, got_label_ref, send_ref, sem, label_sem,
):
    share = pos_ref.shape[1] // n_gy
    gy = lax.axis_index("gy")
    mesh_id = pl.DeviceIdType.MESH
    barrier = pltpu.get_barrier_semaphore()
    for off in range(1, n_gy):
        pl.semaphore_signal(
            barrier, inc=1, device_id={"gy": lax.rem(gy + off, n_gy)}, device_id_type=mesh_id
        )

    def block_copy(off):
        peer = lax.rem(gy + off, n_gy)
        return pltpu.make_async_remote_copy(
            src_ref=send_ref.at[pl.ds(peer * share, share)], dst_ref=got_ref.at[pl.ds(gy * share, share)],
            send_sem=sem.at[0, off - 1], recv_sem=sem.at[1, off - 1],
            device_id={"gy": peer}, device_id_type=mesh_id,
        )

    def label_copy(off):
        peer = lax.rem(gy + off, n_gy)
        return pltpu.make_async_remote_copy(
            src_ref=label_ref.at[peer], dst_ref=got_label_ref.at[gy],
            send_sem=label_sem.at[0, off - 1], recv_sem=label_sem.at[1, off - 1],
            device_id={"gy": peer}, device_id_type=mesh_id,
        )

    def pack(dst, start):
        def some(index, carry):
            held = []
            for u in range(4):
                b = sorting_ref[start + index * 4 + u]
                rows = [ref[c, pl.ds(b, 1), :] for ref in (pos_ref, vel_ref) for c in range(3)]
                held.append(jnp.concatenate(rows + [coef_ref[b]], axis=0))
            for u in range(4):
                dst[start + index * 4 + u] = held[u]
            return carry

        lax.fori_loop(0, share // 4, some, 0)

    order = sorted(range(1, n_gy), key=lambda off: -min(off, n_gy - off))
    for place, off in enumerate(order):
        pack(send_ref, lax.rem(gy + off, n_gy) * share)
        if place == 0:
            pl.semaphore_wait(barrier, n_gy - 1)
            for other in order:
                label_copy(other).start()
        block_copy(off).start()
    pack(got_ref, gy * share)
    got_label_ref[gy] = label_ref[gy]
    for off in order:
        label_copy(off).wait()
    for off in order:
        block_copy(off).wait()


def run_send(sorting, pos, vel, coef, label):
    n_gy = lax.axis_size("gy")
    elems = pos.shape[1]
    f32 = jnp.float32
    dma = pltpu.SemaphoreType.DMA
    return pl.pallas_call(
        functools.partial(send_kernel, n_gy),
        out_shape=(
            jax.ShapeDtypeStruct((elems, 8, 128), f32),
            jax.ShapeDtypeStruct(label.shape, f32),
        ),
        in_specs=[pl.BlockSpec(memory_space=SMEM)] + [pl.BlockSpec(memory_space=VMEM)] * 4,
        out_specs=[pl.BlockSpec(memory_space=VMEM)] * 2,
        scratch_shapes=[
            pltpu.VMEM((elems, 8, 128), f32),
            dma((2, n_gy - 1)),
            dma((2, n_gy - 1)),
        ],
        compiler_params=pltpu.CompilerParams(
            vmem_limit_bytes=32 * 1024 * 1024, collective_id=1, has_side_effects=True
        ),
        name="migrate",
    )(sorting, pos, vel, coef, label)


def inverse_of(position):
    n = position.shape[0]
    ladder = jnp.arange(n, dtype=jnp.int32)
    return jnp.sum(jnp.where(position[None, :] == ladder[:, None], ladder[None, :], 0), axis=1)


def body(velocity, part_pos, part_vel, part_coef, counts, dest, elem):
    _, exd, eyd, ez, nodes = velocity.shape
    elems = exd * eyd * ez
    devices = lax.axis_size("gy")
    share = elems // devices
    f32 = jnp.float32
    ladder = jnp.arange(elems, dtype=jnp.int32)
    earlier = (dest[None, :] == dest[:, None]) & (ladder[None, :] < ladder[:, None])
    position = dest * share + jnp.sum(earlier.astype(jnp.int32), axis=1)
    sorting = inverse_of(position)
    lanes = max(128, share)
    tags = elem * 256 + counts
    room = (position // share) * lanes + position % share
    cells = jnp.arange(devices * lanes, dtype=jnp.int32)
    label = jnp.sum(jnp.where(room[None, :] == cells[:, None], tags[None, :], 0), axis=1)
    got, got_label = run_send(
        sorting, part_pos.transpose(1, 0, 2), part_vel.transpose(1, 0, 2), part_coef,
        label.astype(f32).reshape(devices, 1, lanes),
    )
    got_labels = got_label[:, 0, :share].reshape(elems).astype(jnp.int32)
    slot = inverse_of(got_labels // 256)
    field, far_lo, far_hi, ret = run_main(
        slot, got_labels % 256, got_labels // 256, got,
        velocity.reshape(3, elems, nodes), (exd, eyd, ez),
    )
    source, drag_out = run_yz(position, field, far_lo, far_hi, ret)
    return (drag_out.transpose(1, 0, 2), source)


def solution(mesh):
    in_specs = (
        P(None, "gx", "gy", None, None),
        P(("gx", "gy"), None, None),
        P(("gx", "gy"), None, None),
        P(("gx", "gy"), None, None),
        P(("gx", "gy")),
        P(("gx", "gy")),
        P(("gx", "gy")),
    )
    out_specs = (P(("gx", "gy"), None, None), P(None, "gx", "gy", None, None))
    return jax.shard_map(body, mesh=mesh, in_specs=in_specs, out_specs=out_specs, check_vma=False)
```

```python
import functools

import jax
import jax.numpy as jnp
from jax import lax
from jax.experimental import pallas as pl
from jax.experimental.pallas import tpu as pltpu
from jax.sharding import PartitionSpec as P

GLL = (
    -1.0,
    -0.8717401485096066,
    -0.5917001814331423,
    -0.2092992179024789,
    0.2092992179024789,
    0.5917001814331423,
    0.8717401485096066,
    1.0,
)
SHARPNESS = 8.0
VMEM = pltpu.VMEM
SMEM = pltpu.SMEM
ROWS = 24


def lane_iota(shape):
    return lax.broadcasted_iota(jnp.int32, shape, len(shape) - 1)


def node_consts():
    row = lax.broadcasted_iota(jnp.int32, (8, 128), 0)

    def pick(values):
        out = jnp.full((8, 128), values[7], jnp.float32)
        for i in range(7):
            out = jnp.where(row == i, jnp.float32(values[i]), out)
        return out

    others = [pick([[GLL[m] for m in range(8) if m != i][n] for i in range(8)]) for n in range(7)]
    scales = []
    for i in range(8):
        product = 1.0
        for m in range(8):
            if m != i:
                product *= GLL[i] - GLL[m]
        scales.append(1.0 / product)
    return pick(GLL), others, pick(scales)


def lagrange(x, others, scale):
    diffs = [x - o for o in others]
    left = (diffs[0] * diffs[1]) * (diffs[2] * diffs[3])
    right = (diffs[4] * diffs[5]) * (diffs[6] * scale)
    return left * right


def gauss(x, nodes):
    gap = nodes - x
    return jnp.exp(-SHARPNESS * gap * gap)


def split(x):
    high = x.astype(jnp.bfloat16)
    low = (x - high.astype(jnp.float32)).astype(jnp.bfloat16)
    return high, low


def planes(a, b):
    return jnp.concatenate([a[j : j + 1] * b for j in range(8)], axis=0)


def spread_nodes(vel_ref, vs_ref, elems):
    low = lane_iota((elems, 128)) < 64
    for c in range(3):
        for q in range(4):
            x = vel_ref[c, :, q * 128 : (q + 1) * 128].astype(jnp.float32)
            turned = pltpu.roll(x, 64, 1)
            vs_ref[pl.ds(c * 8 + 2 * q, elems, stride=ROWS), :] = jnp.where(low, x, turned)
            vs_ref[pl.ds(c * 8 + 2 * q + 1, elems, stride=ROWS), :] = jnp.where(low, turned, x)


def st_planes(s, t, nodes):
    high, low = split(planes(gauss(s, nodes), gauss(t, nodes)))
    gathered = jnp.concatenate([high, low], axis=0)
    return jnp.concatenate([gathered, gathered], axis=1)


def project(left, gathered):
    high, low = split(left)
    return lax.dot_general(
        jnp.concatenate([high, low], axis=1),
        gathered,
        (((1,), (1,)), ((), ())),
        preferred_element_type=jnp.float32,
    )


def element(block, count, field, consts, inner_minus, inner_plus):
    nodes, others, scale = consts
    r, s, t = (jnp.broadcast_to(block[d : d + 1], (8, 128)) for d in range(3))
    basis_r = lagrange(r, others, scale)
    basis_st = planes(lagrange(s, others, scale), lagrange(t, others, scale))
    high, low = split(basis_st)
    partial = jnp.dot(
        field.astype(jnp.bfloat16),
        jnp.concatenate([high, low], axis=0),
        preferred_element_type=jnp.float32,
    )
    rel = []
    for c in range(3):
        fluid = jnp.sum(partial[c * 8 : c * 8 + 8] * basis_r, axis=0, keepdims=True)
        rel.append(fluid - block[3 + c : 4 + c])
    speed = jnp.sqrt(rel[0] * rel[0] + rel[1] * rel[1] + rel[2] * rel[2])
    power = jnp.exp(0.687 * jnp.log(block[7:8] * speed))
    factor = block[6:7] * (1.0 + 0.15 * power)
    factor = jnp.where(lane_iota((1, 128)) < count, factor, 0.0)
    drag = [factor * w for w in rel]
    whole = jnp.concatenate(drag, axis=0)
    minus = gauss(r + 2.0, nodes)
    plus = gauss(r - 2.0, nodes)
    weights = [gauss(r, nodes)]
    if inner_minus:
        weights.append(minus)
    if inner_plus:
        weights.append(plus)
    rows = [(-d) * w for w in weights for d in drag]
    blank = jnp.zeros((5, 128), jnp.float32)
    if not inner_minus:
        rows.append(jnp.concatenate([-whole * minus[7:8], blank], axis=0))
    if not inner_plus:
        rows.append(jnp.concatenate([-whole * plus[0:1], blank], axis=0))
    out = project(jnp.concatenate(rows, axis=0), st_planes(s, t, nodes))
    parts, at = {}, ROWS
    parts["own"] = out[0:ROWS]
    for name, inner in (("minus", inner_minus), ("plus", inner_plus)):
        if inner:
            parts[name] = out[at : at + ROWS]
            at += ROWS
    for name, inner in (("minus", inner_minus), ("plus", inner_plus)):
        if not inner:
            parts[name] = out[at : at + 8]
            at += 8
    return whole, parts


def main_kernel(
    shape, chunks, n_gx, n_gy,
    slot_ref, count_ref, elem_ref, got_ref, vel_ref,
    field_ref, far_lo_ref, far_hi_ref, ret_ref,
    vs_ref, ts_ref, fs_ref, drag_ref, pos_ref, gpos_ref, gdrag_ref,
    face_ref, gface_ref, lo_ref, hi_ref, back_ref,
    pos_sem, drag_sem, face_sem, y_sem, back_sem,
):
    exd, eyd, ez = shape
    elems = exd * eyd * ez
    columns = eyd * ez
    share = elems // n_gy
    wide = columns // chunks
    group = min(8, wide)
    turns = columns // group
    per = turns // chunks
    half = columns // 2
    gx = lax.axis_index("gx")
    gy = lax.axis_index("gy")
    has = (gx > 0, gx < n_gx - 1)
    mesh_id = pl.DeviceIdType.MESH

    def to_side(side, src, dst, sems, *at):
        return pltpu.make_async_remote_copy(
            src_ref=src, dst_ref=dst,
            send_sem=sems.at[(0, side) + at], recv_sem=sems.at[(1, 1 - side) + at],
            device_id={"gx": gx - 1 if side == 0 else gx + 1}, device_id_type=mesh_id,
        )

    def from_side(side, src, dst, sems, *at):
        return pltpu.make_async_remote_copy(
            src_ref=src, dst_ref=dst,
            send_sem=sems.at[(0, side) + at], recv_sem=sems.at[(1, side) + at],
            device_id={"gx": gx - 1 if side == 0 else gx + 1}, device_id_type=mesh_id,
        )

    barrier = pltpu.get_barrier_semaphore()
    for side in range(2):
        @pl.when(has[side])
        def _():
            pl.semaphore_signal(
                barrier, inc=1, device_id={"gx": gx - 1 if side == 0 else gx + 1}, device_id_type=mesh_id
            )
    for off in range(1, n_gy):
        pl.semaphore_signal(
            barrier, inc=1, device_id={"gy": lax.rem(gy + off, n_gy)}, device_id_type=mesh_id
        )

    base = (0, elems - columns)

    def stage(index, carry):
        spots = [(side, index * 4 + u) for side in range(2) for u in range(4)]
        held = [got_ref[slot_ref[base[side] + col], 0:3] for side, col in spots]
        for (side, col), value in zip(spots, held):
            pos_ref[side, col] = value
        return carry

    lax.fori_loop(0, columns // 4, stage, 0)
    pl.semaphore_wait(
        barrier, n_gy - 1 + (gx > 0).astype(jnp.int32) + (gx < n_gx - 1).astype(jnp.int32)
    )
    for side in range(2):
        @pl.when(has[side])
        def _():
            to_side(side, pos_ref.at[side], gpos_ref.at[1 - side], pos_sem).start()

    spread_nodes(vel_ref, vs_ref, elems)
    consts = node_consts()
    nodes = consts[0]

    def drag_copy(make, side, chunk):
        start = base[side] + chunk * wide
        return make(
            side, drag_ref.at[pl.ds(start, wide)], gdrag_ref.at[1 - side, pl.ds(chunk * wide, wide)], drag_sem, chunk
        )

    def turn(index, carry):
        for g in range(group):
            col = index * group + g
            parts = []
            for x in range(exd):
                e = x * columns + col
                slot = slot_ref[e]
                drag, part = element(
                    got_ref[slot],
                    count_ref[slot],
                    vs_ref[pl.ds(pl.multiple_of(e * ROWS, 8), ROWS), :],
                    consts,
                    x > 0,
                    x + 1 < exd,
                )
                drag_ref[e] = drag
                parts.append(part)
            for x in range(exd):
                e = x * columns + col
                own = parts[x]["own"]
                if x + 1 < exd:
                    own = own + parts[x + 1]["minus"]
                if x > 0:
                    own = own + parts[x - 1]["plus"]
                ts_ref[pl.ds(pl.multiple_of(e * ROWS, 8), ROWS), :] = own
            start = pl.multiple_of(col * 8, 8)
            fs_ref[0, pl.ds(start, 8), :] = parts[0]["minus"]
            fs_ref[1, pl.ds(start, 8), :] = parts[exd - 1]["plus"]
        for side in range(2):
            @pl.when((lax.rem(index, per) == per - 1) & has[side])
            def _():
                drag_copy(to_side, side, lax.div(index, per)).start()
        return carry

    lax.fori_loop(0, turns, turn, 0)

    def doubled(x):
        return x + pltpu.roll(x, 64, 1)

    low_h = lane_iota((half, 128)) < 64
    for side in range(2):
        node = 0 if side == 0 else 7
        for c in range(3):
            one = doubled(ts_ref[pl.ds(base[side] * ROWS + c * 8 + node, half, stride=ROWS), :])
            two = doubled(ts_ref[pl.ds((base[side] + half) * ROWS + c * 8 + node, half, stride=ROWS), :])
            face_ref[side, c] = jnp.where(low_h, one, two)
        @pl.when(has[side])
        def _():
            to_side(side, face_ref.at[side], gface_ref.at[1 - side], face_sem).start()

    def fill(index, carry):
        held = [drag_ref[elem_ref[index * 8 + u]] for u in range(8)]
        for u in range(8):
            back_ref[index * 8 + u] = held[u]
        return carry

    lax.fori_loop(0, elems // 8, fill, 0)

    def back_copy(off):
        peer = lax.rem(gy + off, n_gy)
        return pltpu.make_async_remote_copy(
            src_ref=back_ref.at[pl.ds(peer * share, share)], dst_ref=ret_ref.at[pl.ds(gy * share, share)],
            send_sem=back_sem.at[0, off - 1], recv_sem=back_sem.at[1, off - 1],
            device_id={"gy": peer}, device_id_type=mesh_id,
        )

    for off in range(1, n_gy):
        back_copy(off).start()

    mine = pl.ds(gy * share, share)
    ret_ref[mine] = back_ref[mine]

    for side in range(2):
        @pl.when(has[side])
        def _():
            from_side(side, pos_ref.at[side], gpos_ref.at[side], pos_sem).wait()

        def ghost(chunk, carry):
            from_side(
                side, drag_ref.at[pl.ds(base[side] + chunk * wide, wide)],
                gdrag_ref.at[side, pl.ds(chunk * wide, wide)], drag_sem, chunk,
            ).wait()
            sums = []
            for g in range(wide):
                col = chunk * wide + g
                place = gpos_ref[side, col]
                force = gdrag_ref[side, col]
                r, s, t = (jnp.broadcast_to(place[d : d + 1], (8, 128)) for d in range(3))
                weight = gauss(r + (-2.0 if side == 0 else 2.0), nodes)
                rows = [(-force[c : c + 1]) * weight for c in range(3)]
                add = project(jnp.concatenate(rows, axis=0), st_planes(s, t, nodes))
                spot = pl.ds(pl.multiple_of((base[side] + col) * ROWS, 8), ROWS)
                sums.append((spot, ts_ref[spot, :] + add))
            for spot, value in sums:
                ts_ref[spot, :] = value
            return carry

        @pl.when(has[side])
        def _():
            lax.fori_loop(0, chunks, ghost, 0)

    for side in range(2):
        @pl.when(has[side])
        def _():
            from_side(side, face_ref.at[side], gface_ref.at[side], face_sem).wait()

    low = lane_iota((ez, 128)) < 64
    spot64 = lane_iota((ez, 128)) % 64

    def lanes(c, x, y, q):
        start = ((x * eyd + y) * ez) * ROWS + c * 8 + 2 * q
        even = ts_ref[pl.ds(start, ez, stride=ROWS), :]
        odd = ts_ref[pl.ds(start + 1, ez, stride=ROWS), :]
        return jnp.where(low, even, odd) + pltpu.roll(jnp.where(low, odd, even), 64, 1)

    def far(side, c, y):
        col = y * ez
        upper = col >= half
        row = col - half if upper else col
        came = gface_ref[side, c, row : row + ez, :]
        turned = pltpu.roll(came, 64, 1)
        came = jnp.where(low, turned, came) if upper else jnp.where(low, came, turned)
        mine = doubled(fs_ref[side, pl.ds(col * 8 + c, ez, stride=8), :])
        return jnp.where(has[side], came + mine, 0.0)

    for y in (0, eyd - 1) + tuple(range(1, eyd - 1)):
        for c in range(3):
            grid = [[lanes(c, x, y, q) for q in range(4)] for x in range(exd)]
            for x in range(exd):
                above = pltpu.roll(grid[x + 1][0], 64, 1) if x + 1 < exd else far(1, c, y)
                below = pltpu.roll(grid[x - 1][3], 64, 1) if x > 0 else far(0, c, y)
                done = list(grid[x])
                done[3] = done[3] + jnp.where(low, 0.0, above)
                done[0] = done[0] + jnp.where(low, below, 0.0)
                for q in range(4):
                    field_ref[c, x, y, :, q * 128 : (q + 1) * 128] = done[q]
                if y == 0:
                    face = jnp.where(spot64 < 8, done[0], 0.0)
                    for q in range(1, 4):
                        face = face + pltpu.roll(jnp.where(spot64 < 8, done[q], 0.0), 8 * q, 1)
                    lo_ref[c, x] = face
                if y == eyd - 1:
                    face = jnp.where(spot64 >= 56, done[0], 0.0)
                    for q in range(1, 4):
                        face = face + pltpu.roll(jnp.where(spot64 >= 56, done[q], 0.0), 128 - 8 * q, 1)
                    hi_ref[c, x] = face
        if y == eyd - 1:
            lo_copy = pltpu.make_async_remote_copy(
                src_ref=lo_ref, dst_ref=far_lo_ref, send_sem=y_sem.at[0, 0], recv_sem=y_sem.at[1, 0],
                device_id={"gy": gy - 1}, device_id_type=mesh_id,
            )
            hi_copy = pltpu.make_async_remote_copy(
                src_ref=hi_ref, dst_ref=far_hi_ref, send_sem=y_sem.at[0, 1], recv_sem=y_sem.at[1, 1],
                device_id={"gy": gy + 1}, device_id_type=mesh_id,
            )
            @pl.when(gy > 0)
            def _():
                lo_copy.start()
            @pl.when(gy < n_gy - 1)
            def _():
                hi_copy.start()

    @pl.when(gy > 0)
    def _():
        lo_copy.wait_send()
        hi_copy.wait_recv()
    @pl.when(gy < n_gy - 1)
    def _():
        hi_copy.wait_send()
        lo_copy.wait_recv()
    for off in range(1, n_gy):
        back_copy(off).wait()


def run_main(slot, count, elem_of, got, velocity, shape):
    exd, eyd, ez = shape
    elems = exd * eyd * ez
    columns = eyd * ez
    n_gx, n_gy = lax.axis_size("gx"), lax.axis_size("gy")
    chunks = 4
    f32 = jnp.float32
    dma = pltpu.SemaphoreType.DMA
    face = (3, exd, ez, 128)
    return pl.pallas_call(
        functools.partial(main_kernel, shape, chunks, n_gx, n_gy),
        out_shape=(
            jax.ShapeDtypeStruct((3, exd, eyd, ez, 512), f32),
            jax.ShapeDtypeStruct(face, f32),
            jax.ShapeDtypeStruct(face, f32),
            jax.ShapeDtypeStruct((elems, 3, 128), f32),
        ),
        in_specs=[pl.BlockSpec(memory_space=SMEM)] * 3 + [pl.BlockSpec(memory_space=VMEM)] * 2,
        out_specs=[pl.BlockSpec(memory_space=VMEM)] * 4,
        scratch_shapes=[
            pltpu.VMEM((elems * ROWS, 128), f32),
            pltpu.VMEM((elems * ROWS, 128), f32),
            pltpu.VMEM((2, columns * 8, 128), f32),
            pltpu.VMEM((elems, 3, 128), f32),
            pltpu.VMEM((2, columns, 3, 128), f32),
            pltpu.VMEM((2, columns, 3, 128), f32),
            pltpu.VMEM((2, columns, 3, 128), f32),
            pltpu.VMEM((2, 3, columns // 2, 128), f32),
            pltpu.VMEM((2, 3, columns // 2, 128), f32),
            pltpu.VMEM(face, f32),
            pltpu.VMEM(face, f32),
            pltpu.VMEM((elems, 3, 128), f32),
            dma((2, 2)),
            dma((2, 2, chunks)),
            dma((2, 2)),
            dma((2, 2)),
            dma((2, n_gy - 1)),
        ],
        compiler_params=pltpu.CompilerParams(
            vmem_limit_bytes=48 * 1024 * 1024, collective_id=0, has_side_effects=True
        ),
        cost_estimate=pl.CostEstimate(flops=200_000_000, bytes_accessed=4_000_000, transcendentals=700_000),
        name="elements",
    )(slot, count, elem_of, got, velocity)


def yz_pass(position_ref, field_ref, far_lo_ref, far_hi_ref, ret_ref, out_ref, drag_ref, buf_ref, sem):
    _, exd, eyd, ez, _ = field_ref.shape
    at = lax.axis_index("gy")
    first = at > 0
    last = at < lax.axis_size("gy") - 1
    place = lane_iota((ez, 128)) % 64
    k = lane_iota((ez, 128)) % 8
    row = lax.broadcasted_iota(jnp.int32, (ez, 128), 0)
    up = (k == 7) & (row < ez - 1)
    down = (k == 0) & (row > 0)
    copies = []
    for c in range(3):
        for x in range(exd):
            far_lo = jnp.where(last, far_lo_ref[c, x], 0.0)
            far_hi = jnp.where(first, far_hi_ref[c, x], 0.0)
            for q in range(4):
                spot = slice(q * 128, (q + 1) * 128)
                cells = [field_ref[c, x, y, :, spot] for y in range(eyd)]
                for y in range(eyd):
                    if y + 1 < eyd:
                        above = pltpu.roll(cells[y + 1], 56, 1)
                    else:
                        above = pltpu.roll(far_lo, (56 - 8 * q) % 128, 1)
                    if y > 0:
                        below = pltpu.roll(cells[y - 1], 72, 1)
                    else:
                        below = pltpu.roll(far_hi, (72 + 8 * q) % 128, 1)
                    v = cells[y] + jnp.where(place >= 56, above, 0.0) + jnp.where(place < 8, below, 0.0)
                    nxt = pltpu.roll(pltpu.roll(v, ez - 1, 0), 7, 1)
                    prv = pltpu.roll(pltpu.roll(v, 1, 0), 121, 1)
                    buf_ref[c, x, y, :, spot] = v + jnp.where(up, nxt, 0.0) + jnp.where(down, prv, 0.0)


            copies.append(pltpu.make_async_copy(buf_ref.at[c, x], out_ref.at[c, x], sem.at[c, x]))
            copies[-1].start()

    def pick(index, carry):
        held = [ret_ref[position_ref[index * 8 + u]] for u in range(8)]
        for c in range(3):
            rows = jnp.concatenate([h[c : c + 1] for h in held], axis=0)
            drag_ref[c, pl.ds(pl.multiple_of(index * 8, 8), 8), :] = rows
        return carry

    lax.fori_loop(0, ret_ref.shape[0] // 8, pick, 0)
    for copy in copies:
        copy.wait()


def run_yz(position, field, far_lo, far_hi, ret):
    f32 = jnp.float32
    return pl.pallas_call(
        yz_pass,
        out_shape=(jax.ShapeDtypeStruct(field.shape, f32), jax.ShapeDtypeStruct((3, ret.shape[0], 128), f32)),
        in_specs=[pl.BlockSpec(memory_space=SMEM)] + [pl.BlockSpec(memory_space=VMEM)] * 4,
        out_specs=[pl.BlockSpec(memory_space=pl.ANY), pl.BlockSpec(memory_space=VMEM)],
        scratch_shapes=[pltpu.VMEM(field.shape, f32), pltpu.SemaphoreType.DMA(field.shape[:2])],
        compiler_params=pltpu.CompilerParams(vmem_limit_bytes=32 * 1024 * 1024),
        name="yzpass",
    )(position, field, far_lo, far_hi, ret)


def send_kernel(
    n_gy, sorting_ref, pos_ref, vel_ref, coef_ref, label_ref,
    got_ref, got_label_ref, send_ref, sem, label_sem,
):
    share = pos_ref.shape[1] // n_gy
    gy = lax.axis_index("gy")
    mesh_id = pl.DeviceIdType.MESH
    barrier = pltpu.get_barrier_semaphore()
    for off in range(1, n_gy):
        pl.semaphore_signal(
            barrier, inc=1, device_id={"gy": lax.rem(gy + off, n_gy)}, device_id_type=mesh_id
        )

    def block_copy(off):
        peer = lax.rem(gy + off, n_gy)
        return pltpu.make_async_remote_copy(
            src_ref=send_ref.at[pl.ds(peer * share, share)], dst_ref=got_ref.at[pl.ds(gy * share, share)],
            send_sem=sem.at[0, off - 1], recv_sem=sem.at[1, off - 1],
            device_id={"gy": peer}, device_id_type=mesh_id,
        )

    def label_copy(off):
        peer = lax.rem(gy + off, n_gy)
        return pltpu.make_async_remote_copy(
            src_ref=label_ref.at[peer], dst_ref=got_label_ref.at[gy],
            send_sem=label_sem.at[0, off - 1], recv_sem=label_sem.at[1, off - 1],
            device_id={"gy": peer}, device_id_type=mesh_id,
        )

    def pack(dst, start):
        def some(index, carry):
            held = []
            for u in range(4):
                b = sorting_ref[start + index * 4 + u]
                rows = [ref[c, pl.ds(b, 1), :] for ref in (pos_ref, vel_ref) for c in range(3)]
                held.append(jnp.concatenate(rows + [coef_ref[b]], axis=0))
            for u in range(4):
                dst[start + index * 4 + u] = held[u]
            return carry

        lax.fori_loop(0, share // 4, some, 0)

    order = sorted(range(1, n_gy), key=lambda off: -min(off, n_gy - off))
    for place, off in enumerate(order):
        pack(send_ref, lax.rem(gy + off, n_gy) * share)
        if place == 0:
            pl.semaphore_wait(barrier, n_gy - 1)
            for other in order:
                label_copy(other).start()
        block_copy(off).start()
    pack(got_ref, gy * share)
    got_label_ref[gy] = label_ref[gy]
    for off in order:
        label_copy(off).wait()
    for off in order:
        block_copy(off).wait()


def run_send(sorting, pos, vel, coef, label):
    n_gy = lax.axis_size("gy")
    elems = pos.shape[1]
    f32 = jnp.float32
    dma = pltpu.SemaphoreType.DMA
    return pl.pallas_call(
        functools.partial(send_kernel, n_gy),
        out_shape=(
            jax.ShapeDtypeStruct((elems, 8, 128), f32),
            jax.ShapeDtypeStruct(label.shape, f32),
        ),
        in_specs=[pl.BlockSpec(memory_space=SMEM)] + [pl.BlockSpec(memory_space=VMEM)] * 4,
        out_specs=[pl.BlockSpec(memory_space=VMEM)] * 2,
        scratch_shapes=[
            pltpu.VMEM((elems, 8, 128), f32),
            dma((2, n_gy - 1)),
            dma((2, n_gy - 1)),
        ],
        compiler_params=pltpu.CompilerParams(
            vmem_limit_bytes=32 * 1024 * 1024, collective_id=1, has_side_effects=True
        ),
        name="migrate",
    )(sorting, pos, vel, coef, label)


def inverse_of(position):
    n = position.shape[0]
    ladder = jnp.arange(n, dtype=jnp.int32)
    return jnp.sum(jnp.where(position[None, :] == ladder[:, None], ladder[None, :], 0), axis=1)


def body(velocity, part_pos, part_vel, part_coef, counts, dest, elem):
    _, exd, eyd, ez, nodes = velocity.shape
    elems = exd * eyd * ez
    devices = lax.axis_size("gy")
    share = elems // devices
    f32 = jnp.float32
    ladder = jnp.arange(elems, dtype=jnp.int32)
    earlier = (dest[None, :] == dest[:, None]) & (ladder[None, :] < ladder[:, None])
    position = dest * share + jnp.sum(earlier.astype(jnp.int32), axis=1)
    sorting = inverse_of(position)
    lanes = max(128, share)
    tags = elem * 256 + counts
    room = (position // share) * lanes + position % share
    cells = jnp.arange(devices * lanes, dtype=jnp.int32)
    label = jnp.sum(jnp.where(room[None, :] == cells[:, None], tags[None, :], 0), axis=1)
    got, got_label = run_send(
        sorting, part_pos.transpose(1, 0, 2), part_vel.transpose(1, 0, 2), part_coef,
        label.astype(f32).reshape(devices, 1, lanes),
    )
    got_labels = got_label[:, 0, :share].reshape(elems).astype(jnp.int32)
    slot = inverse_of(got_labels // 256)
    field, far_lo, far_hi, ret = run_main(
        slot, got_labels % 256, got_labels // 256, got,
        velocity.reshape(3, elems, nodes), (exd, eyd, ez),
    )
    source, drag_out = run_yz(position, field, far_lo, far_hi, ret)
    return (drag_out.transpose(1, 0, 2), source)


def solution(mesh):
    in_specs = (
        P(None, "gx", "gy", None, None),
        P(("gx", "gy"), None, None),
        P(("gx", "gy"), None, None),
        P(("gx", "gy"), None, None),
        P(("gx", "gy")),
        P(("gx", "gy")),
        P(("gx", "gy")),
    )
    out_specs = (P(("gx", "gy"), None, None), P(None, "gx", "gy", None, None))
    return jax.shard_map(body, mesh=mesh, in_specs=in_specs, out_specs=out_specs, check_vma=False)
```
